128 devices in a mesh: data: 1, fsdp: 16 (over z, y), ep: 8 (over x, core).
Axes of the slice: x: 4, y: 4, z: 4, core: 2. Of those that a mesh axis runs over, the one named last changes fastest.
Arguments:
- x_in: bfloat16 [128, 384, 2048], P(('data', 'fsdp', 'ep'))
- w_qkv: bfloat16 [2048, 6144], P('fsdp')
- w_out: bfloat16 [2048, 2048], P('fsdp')
- w_gate: bfloat16 [64, 2048, 1408], P('ep', 'fsdp')
- w_up: bfloat16 [64, 2048, 1408], P('ep', 'fsdp')
- w_down: bfloat16 [64, 1408, 2048], P('ep', None, 'fsdp')
- ws_gate: bfloat16 [2048, 2816], P('fsdp')
- ws_up: bfloat16 [2048, 2816], P('fsdp')
- ws_down: bfloat16 [2816, 2048], P(None, 'fsdp')
- expert_ids: int32 [128, 384, 6], P(('data', 'fsdp', 'ep'))
- slot_ids: int32 [128, 384, 6], P(('data', 'fsdp', 'ep'))
- gate_vals: bfloat16 [128, 384, 6], P(('data', 'fsdp', 'ep'))
Outputs:
- output: bfloat16 [128, 384, 2048], P(('data', 'fsdp', 'ep'))
All inputs are finite; a program needn't handle non-finite values.
Results may differ from the reference program's by a relative error of at most 0.00961566.
Values are sent between devices in bfloat16 or wider.
A program may use at most 1 GiB of HBM per device.

```python
import jax
import jax.numpy as jnp
from jax import lax

MODEL_DIM = 2048
NUM_HEADS = 16
HEAD_DIM = 128
NUM_EXPERTS = 64
TOP_K = 6
EXPERT_FF = 1408
SHARED_FF = 2816
BATCH_DEV = 1
SEQ_LEN = 384
GROUP_DEVS = 128
TOKENS = BATCH_DEV * SEQ_LEN
CAPACITY = ((5 * TOKENS * TOP_K) // (4 * NUM_EXPERTS) + 7) // 8 * 8
ROPE_BASE = 10000.0
EPSILON = 1e-6


def normal_weight(rand_key, weight_shape, fan_in):
    scaled = jax.random.normal(rand_key, weight_shape, jnp.float32) * (fan_in ** -0.5)
    return scaled.astype(jnp.bfloat16)


def draw_routing(rand_key):
    score_key, bias_key, hot_key = jax.random.split(rand_key, 3)
    expert_iota = jnp.arange(NUM_EXPERTS, dtype=jnp.int32)
    scores = jax.random.randint(score_key, (GROUP_DEVS, TOKENS, NUM_EXPERTS), 0, 1000, dtype=jnp.int32)
    expert_bias = jax.random.randint(bias_key, (GROUP_DEVS, 1, NUM_EXPERTS), 0, 500, dtype=jnp.int32)
    hot_expert = jax.random.randint(hot_key, (GROUP_DEVS, 1, 1), 0, NUM_EXPERTS, dtype=jnp.int32)
    total_score = scores + expert_bias + jnp.where(expert_iota == hot_expert, 2000, 0)
    ranked = total_score * NUM_EXPERTS + expert_iota
    chosen = lax.top_k(ranked, TOP_K)[1].astype(jnp.int32)
    flat_ids = chosen.reshape(GROUP_DEVS, TOKENS * TOP_K)

    def device_slots(dev_ids):
        onehot = (dev_ids[:, None] == expert_iota[None, :]).astype(jnp.int32)
        running = jnp.cumsum(onehot, axis=0) - 1
        position = jnp.sum(running * onehot, axis=1)
        return jnp.where(position < CAPACITY, position, -1)

    slot_table = lax.map(device_slots, flat_ids)
    route_shape = (GROUP_DEVS * BATCH_DEV, SEQ_LEN, TOP_K)
    return chosen.reshape(route_shape), slot_table.reshape(route_shape)


def setup_inputs(seed: int = 0, part: int = 0) -> dict:
    weight_keys = jax.random.split(jax.random.key(seed), 8)
    part_keys = jax.random.split(jax.random.fold_in(jax.random.key(seed + 1), part), 3)
    n_seqs = GROUP_DEVS * BATCH_DEV
    expert_ids, slot_ids = draw_routing(part_keys[1])
    x_in = jax.random.normal(part_keys[0], (n_seqs, SEQ_LEN, MODEL_DIM), jnp.float32).astype(jnp.bfloat16)
    gate_vals = jax.random.uniform(part_keys[2], (n_seqs, SEQ_LEN, TOP_K), jnp.float32, 0.25, 1.0).astype(jnp.bfloat16)
    return {"x_in": x_in, "w_qkv": normal_weight(weight_keys[0], (MODEL_DIM, 3 * NUM_HEADS * HEAD_DIM), MODEL_DIM), "w_out": normal_weight(weight_keys[1], (NUM_HEADS * HEAD_DIM, MODEL_DIM), NUM_HEADS * HEAD_DIM), "w_gate": normal_weight(weight_keys[2], (NUM_EXPERTS, MODEL_DIM, EXPERT_FF), MODEL_DIM), "w_up": normal_weight(weight_keys[3], (NUM_EXPERTS, MODEL_DIM, EXPERT_FF), MODEL_DIM), "w_down": normal_weight(weight_keys[4], (NUM_EXPERTS, EXPERT_FF, MODEL_DIM), EXPERT_FF), "ws_gate": normal_weight(weight_keys[5], (MODEL_DIM, SHARED_FF), MODEL_DIM), "ws_up": normal_weight(weight_keys[6], (MODEL_DIM, SHARED_FF), MODEL_DIM), "ws_down": normal_weight(weight_keys[7], (SHARED_FF, MODEL_DIM), SHARED_FF), "expert_ids": expert_ids, "slot_ids": slot_ids, "gate_vals": gate_vals}


def rms_norm(values):
    vals_f32 = values.astype(jnp.float32)
    mean_sq = jnp.mean(vals_f32 * vals_f32, axis=-1, keepdims=True)
    return (vals_f32 * lax.rsqrt(mean_sq + EPSILON)).astype(jnp.bfloat16)


def rotary_embed(heads_in, positions):
    half_dim = HEAD_DIM // 2
    inv_freq = ROPE_BASE ** (-jnp.arange(half_dim).astype(jnp.float32) * (2.0 / HEAD_DIM))
    angles = positions[:, None] * inv_freq[None, :]
    cos_tab = jnp.cos(angles)[:, None, :]
    sin_tab = jnp.sin(angles)[:, None, :]
    vals_f32 = heads_in.astype(jnp.float32)
    first_half = vals_f32[..., :half_dim]
    second_half = vals_f32[..., half_dim:]
    rotated = jnp.concatenate([first_half * cos_tab - second_half * sin_tab, second_half * cos_tab + first_half * sin_tab], axis=-1)
    return rotated.astype(jnp.bfloat16)


def attention_block(x_dev, w_qkv, w_out):
    normed = rms_norm(x_dev).reshape(TOKENS, MODEL_DIM)
    qkv_proj = jnp.dot(normed, w_qkv, preferred_element_type=jnp.float32).astype(jnp.bfloat16)
    qkv_proj = qkv_proj.reshape(BATCH_DEV, SEQ_LEN, 3, NUM_HEADS, HEAD_DIM)
    positions = jnp.arange(SEQ_LEN).astype(jnp.float32)
    query_rot = rotary_embed(qkv_proj[:, :, 0], positions).astype(jnp.float32)
    key_rot = rotary_embed(qkv_proj[:, :, 1], positions).astype(jnp.float32)
    value_heads = qkv_proj[:, :, 2].astype(jnp.float32)
    scores = jnp.einsum("bqhd,bkhd->bhqk", query_rot, key_rot) * (HEAD_DIM ** -0.5)
    causal = jnp.arange(SEQ_LEN)[:, None] >= jnp.arange(SEQ_LEN)[None, :]
    attn_probs = jax.nn.softmax(jnp.where(causal, scores, -1e30), axis=-1).astype(jnp.bfloat16)
    attn_mixed = jnp.einsum("bhqk,bkhd->bqhd", attn_probs.astype(jnp.float32), value_heads).astype(jnp.bfloat16)
    attn_out = jnp.dot(attn_mixed.reshape(TOKENS, NUM_HEADS * HEAD_DIM), w_out, preferred_element_type=jnp.float32)
    return (x_dev.reshape(TOKENS, MODEL_DIM).astype(jnp.float32) + attn_out).astype(jnp.bfloat16)


def expert_rows(operands):
    rows_in, gate_w, up_w, down_w = operands
    gate_act = jnp.dot(rows_in, gate_w, preferred_element_type=jnp.float32)
    up_act = jnp.dot(rows_in, up_w, preferred_element_type=jnp.float32)
    inner_act = (jax.nn.silu(gate_act) * up_act).astype(jnp.bfloat16)
    return jnp.dot(inner_act, down_w, preferred_element_type=jnp.float32).astype(jnp.bfloat16)


def moe_block(hidden, dev_ids, dev_slots, dev_gates, w_gate, w_up, w_down, ws_gate, ws_up, ws_down):
    normed = rms_norm(hidden)
    kept_mask = dev_slots >= 0
    row_index = dev_ids * CAPACITY + dev_slots
    target = jnp.where(kept_mask, row_index, NUM_EXPERTS * CAPACITY).reshape(-1)
    source_tok = jnp.arange(TOKENS * TOP_K, dtype=jnp.int32) // TOP_K
    row_source = jnp.full((NUM_EXPERTS * CAPACITY,), TOKENS, jnp.int32).at[target].set(source_tok, mode="drop")
    buffer = jnp.take(normed, row_source, axis=0, mode="fill", fill_value=0).reshape(NUM_EXPERTS, CAPACITY, MODEL_DIM)
    expert_out = lax.map(expert_rows, (buffer, w_gate, w_up, w_down)).reshape(NUM_EXPERTS * CAPACITY, MODEL_DIM)
    picked = jnp.take(expert_out, jnp.where(kept_mask, row_index, 0), axis=0).astype(jnp.float32)
    weight = jnp.where(kept_mask, dev_gates.astype(jnp.float32), 0.0)
    routed = jnp.sum(weight[:, :, None] * picked, axis=1)
    shared_act = jax.nn.silu(jnp.dot(normed, ws_gate, preferred_element_type=jnp.float32)) * jnp.dot(normed, ws_up, preferred_element_type=jnp.float32)
    shared_out = jnp.dot(shared_act.astype(jnp.bfloat16), ws_down, preferred_element_type=jnp.float32)
    return (hidden.astype(jnp.float32) + shared_out + routed).astype(jnp.bfloat16)


def reference(x_in, w_qkv, w_out, w_gate, w_up, w_down, ws_gate, ws_up, ws_down, expert_ids, slot_ids, gate_vals):
    def per_device(operands):
        x_dev, dev_ids, dev_slots, dev_gates = operands
        hidden = attention_block(x_dev, w_qkv, w_out)
        return moe_block(hidden, dev_ids, dev_slots, dev_gates, w_gate, w_up, w_down, ws_gate, ws_up, ws_down)

    stacked = (x_in.reshape(GROUP_DEVS, BATCH_DEV, SEQ_LEN, MODEL_DIM), expert_ids.reshape(GROUP_DEVS, TOKENS, TOP_K), slot_ids.reshape(GROUP_DEVS, TOKENS, TOP_K), gate_vals.reshape(GROUP_DEVS, TOKENS, TOP_K))
    out_rows = lax.map(per_device, stacked)
    return out_rows.reshape(GROUP_DEVS * BATCH_DEV, SEQ_LEN, MODEL_DIM)
```

```python
import jax
import jax.numpy as jnp
from jax import lax
from jax.sharding import Mesh, PartitionSpec as P

HEAD_DIM = 128
ROPE_BASE = 10000.0
EPSILON = 1e-6
ALL = ("fsdp", "x", "core")
SWAP = [(0, 1), (1, 0)]


def rms_norm(values):
    vals_f32 = values.astype(jnp.float32)
    mean_sq = jnp.mean(vals_f32 * vals_f32, axis=-1, keepdims=True)
    return (vals_f32 * lax.rsqrt(mean_sq + EPSILON)).astype(jnp.bfloat16)


def rotary_embed(heads_in, positions):
    half_dim = HEAD_DIM // 2
    inv_freq = ROPE_BASE ** (-jnp.arange(half_dim, dtype=jnp.float32) * (2.0 / HEAD_DIM))
    angles = positions[:, None] * inv_freq[None, :]
    cos_tab = jnp.cos(angles)[:, None, :]
    sin_tab = jnp.sin(angles)[:, None, :]
    vals_f32 = heads_in.astype(jnp.float32)
    first_half = vals_f32[..., :half_dim]
    second_half = vals_f32[..., half_dim:]
    rotated = jnp.concatenate([first_half * cos_tab - second_half * sin_tab, second_half * cos_tab + first_half * sin_tab], axis=-1)
    return rotated.astype(jnp.bfloat16)


def attention_block(x_in, qkv_weight, out_weight):
    n_batch, seq_len, model_dim = x_in.shape
    n_heads = qkv_weight.shape[1] // (3 * HEAD_DIM)
    normed = rms_norm(x_in)
    qkv_proj = jnp.einsum("bsd,dn->bsn", normed, qkv_weight, preferred_element_type=jnp.float32).astype(jnp.bfloat16)
    qkv_proj = qkv_proj.reshape(n_batch, seq_len, 3, n_heads, HEAD_DIM)
    positions = jnp.arange(seq_len, dtype=jnp.float32)
    query_rot = rotary_embed(qkv_proj[:, :, 0], positions)
    key_rot = rotary_embed(qkv_proj[:, :, 1], positions)
    scores = jnp.einsum("bqhd,bkhd->bhqk", query_rot, key_rot, preferred_element_type=jnp.float32) * (HEAD_DIM ** -0.5)
    causal = jnp.arange(seq_len)[:, None] >= jnp.arange(seq_len)[None, :]
    attn_probs = jax.nn.softmax(jnp.where(causal, scores, -1e30), axis=-1).astype(jnp.bfloat16)
    attn_mixed = jnp.einsum("bhqk,bkhd->bqhd", attn_probs, qkv_proj[:, :, 2], preferred_element_type=jnp.float32).astype(jnp.bfloat16)
    attn_out = jnp.einsum("bsn,nm->bsm", attn_mixed.reshape(n_batch, seq_len, n_heads * HEAD_DIM), out_weight, preferred_element_type=jnp.float32)
    return (x_in.astype(jnp.float32) + attn_out).astype(jnp.bfloat16)


def capacity_for(n_tokens, top_k, n_experts):
    return ((5 * n_tokens * top_k) // (4 * n_experts) + 7) // 8 * 8


def nt_dot(lhs, rhs):
    return lax.dot_general(lhs, rhs, (((1,), (1,)), ((), ())), preferred_element_type=jnp.float32)


def solution(mesh):
    n_f, n_ep = mesh.shape["fsdp"], mesh.shape["ep"]
    n_core = 2
    n_x = n_ep // n_core
    phys = Mesh(mesh.devices.reshape(n_f, n_x, n_core), ALL)
    tok_spec = P(ALL)
    row_spec = P("fsdp", None)
    ep = ("x", "core")

    def gather_rows(shard):
        part = shard.shape[0] // n_ep
        mine = lax.axis_index("x") * n_core + lax.axis_index("core")
        piece = lax.dynamic_slice_in_dim(shard, mine * part, part, 0)
        return lax.all_gather(piece, ALL, axis=0, tiled=True)

    def collect_expert(shard):
        core = lax.axis_index("core")
        n_loc, depth, width = shard.shape
        half = depth // n_core
        keep = lax.dynamic_slice_in_dim(shard, core * half, half, 1)
        give = lax.dynamic_slice_in_dim(shard, (1 - core) * half, half, 1)
        got = lax.ppermute(give, "core", SWAP)
        first = core == 0
        both = jnp.concatenate([jnp.where(first, keep, got), jnp.where(first, got, keep)], axis=0)
        mine = lax.all_to_all(both, "fsdp", 0, 0, tiled=True)
        other = lax.ppermute(mine, "core", SWAP)
        whole = jnp.stack([jnp.where(first, mine, other), jnp.where(first, other, mine)], axis=1)
        return whole.reshape(n_f * depth, width)

    def local_step(x_in, w_qkv, w_out, w_gate, w_up, w_down, ws_gate, ws_up, ws_down, expert_ids, slot_ids, gate_vals):
        n_batch, seq_len, model_dim = x_in.shape
        n_tokens = n_batch * seq_len
        top_k = expert_ids.shape[-1]
        n_experts = w_gate.shape[0] * n_ep
        capacity = capacity_for(n_tokens, top_k, n_experts)
        part = capacity // n_core
        n_rows = n_experts * capacity
        s_ff = ws_gate.shape[1]

        qkv_full = gather_rows(w_qkv)
        out_full = gather_rows(w_out)
        gate_w = collect_expert(w_gate)
        up_w = collect_expert(w_up)
        down_w = collect_expert(jnp.swapaxes(w_down, 1, 2))
        shared_full = gather_rows(jnp.concatenate([ws_gate, ws_up, ws_down.T], axis=1))

        ids = expert_ids.reshape(n_tokens, top_k)
        slots = slot_ids.reshape(n_tokens, top_k)
        gates = gate_vals.reshape(n_tokens, top_k)
        kept = slots >= 0
        dest = ((ids % n_f) * n_x + ids // n_f) * n_core + slots // part
        row = jnp.where(kept, dest * part + slots % part, n_rows)
        source_tok = jnp.arange(n_tokens * top_k, dtype=jnp.int32) // top_k
        row_source = jnp.full((n_rows,), n_tokens, jnp.int32).at[row.reshape(-1)].set(source_tok, mode="drop")
        row_gate = jnp.zeros((n_rows,), gates.dtype).at[row.reshape(-1)].set(gates.reshape(-1), mode="drop")
        tok_iota = jnp.arange(n_tokens, dtype=jnp.int32)
        pick = (row_source[:, None] == tok_iota[None, :])
        spread = pick.astype(jnp.bfloat16)
        merge = jnp.where(row_source[None, :] == tok_iota[:, None], row_gate[None, :], jnp.zeros((), gates.dtype))

        hidden = attention_block(x_in, qkv_full, out_full).reshape(n_tokens, model_dim)
        normed = rms_norm(hidden)
        buffer = jnp.dot(spread, normed, preferred_element_type=jnp.float32).astype(jnp.bfloat16)
        received = lax.all_to_all(buffer.reshape(n_f * n_ep, part, model_dim), ALL, 0, 0, tiled=True)
        rows_in = received.reshape(n_rows, model_dim)
        gate_act = jnp.dot(rows_in, gate_w, preferred_element_type=jnp.float32)
        up_act = jnp.dot(rows_in, up_w, preferred_element_type=jnp.float32)
        inner = (jax.nn.silu(gate_act) * up_act).astype(jnp.bfloat16)
        expert_out = nt_dot(inner, down_w).astype(jnp.bfloat16)
        returned = lax.all_to_all(expert_out.reshape(n_f * n_ep, part, model_dim), ALL, 0, 0, tiled=True)
        routed = jnp.dot(merge, returned.reshape(n_rows, model_dim), preferred_element_type=jnp.float32)

        s_gate = jnp.dot(normed, shared_full[:, :s_ff], preferred_element_type=jnp.float32)
        s_up = jnp.dot(normed, shared_full[:, s_ff:2 * s_ff], preferred_element_type=jnp.float32)
        s_inner = (jax.nn.silu(s_gate) * s_up).astype(jnp.bfloat16)
        shared_out = nt_dot(s_inner, shared_full[:, 2 * s_ff:])
        summed = hidden.astype(jnp.float32) + shared_out + routed
        return summed.astype(jnp.bfloat16).reshape(n_batch, seq_len, model_dim)

    return jax.shard_map(local_step, mesh=phys, in_specs=(tok_spec, row_spec, row_spec, P(ep, "fsdp", None), P(ep, "fsdp", None), P(ep, None, "fsdp"), row_spec, row_spec, P(None, "fsdp"), tok_spec, tok_spec, tok_spec), out_specs=tok_spec, check_vma=False)
```

```python
import jax
import jax.numpy as jnp
from jax import lax
from jax.sharding import Mesh, PartitionSpec as P

HEAD_DIM = 128
ROPE_BASE = 10000.0
EPSILON = 1e-6
ALL = ("fsdp", "x", "core")
SWAP = [(0, 1), (1, 0)]


def rms_norm(values):
    vals_f32 = values.astype(jnp.float32)
    mean_sq = jnp.mean(vals_f32 * vals_f32, axis=-1, keepdims=True)
    return (vals_f32 * lax.rsqrt(mean_sq + EPSILON)).astype(jnp.bfloat16)


def rotary_embed(heads_in, positions):
    half_dim = HEAD_DIM // 2
    inv_freq = ROPE_BASE ** (-jnp.arange(half_dim, dtype=jnp.float32) * (2.0 / HEAD_DIM))
    angles = positions[:, None] * inv_freq[None, :]
    cos_tab = jnp.cos(angles)[:, None, :]
    sin_tab = jnp.sin(angles)[:, None, :]
    vals_f32 = heads_in.astype(jnp.float32)
    first_half = vals_f32[..., :half_dim]
    second_half = vals_f32[..., half_dim:]
    rotated = jnp.concatenate([first_half * cos_tab - second_half * sin_tab, second_half * cos_tab + first_half * sin_tab], axis=-1)
    return rotated.astype(jnp.bfloat16)


def attention_block(x_in, qkv_weight, out_weight):
    n_batch, seq_len, model_dim = x_in.shape
    n_heads = qkv_weight.shape[1] // (3 * HEAD_DIM)
    normed = rms_norm(x_in)
    qkv_proj = jnp.einsum("bsd,dn->bsn", normed, qkv_weight, preferred_element_type=jnp.float32).astype(jnp.bfloat16)
    qkv_proj = qkv_proj.reshape(n_batch, seq_len, 3, n_heads, HEAD_DIM)
    positions = jnp.arange(seq_len, dtype=jnp.float32)
    query_rot = rotary_embed(qkv_proj[:, :, 0], positions)
    key_rot = rotary_embed(qkv_proj[:, :, 1], positions)
    scores = jnp.einsum("bqhd,bkhd->bhqk", query_rot, key_rot, preferred_element_type=jnp.float32) * (HEAD_DIM ** -0.5)
    causal = jnp.arange(seq_len)[:, None] >= jnp.arange(seq_len)[None, :]
    attn_probs = jax.nn.softmax(jnp.where(causal, scores, -1e30), axis=-1).astype(jnp.bfloat16)
    attn_mixed = jnp.einsum("bhqk,bkhd->bqhd", attn_probs, qkv_proj[:, :, 2], preferred_element_type=jnp.float32).astype(jnp.bfloat16)
    attn_out = jnp.einsum("bsn,nm->bsm", attn_mixed.reshape(n_batch, seq_len, n_heads * HEAD_DIM), out_weight, preferred_element_type=jnp.float32)
    return (x_in.astype(jnp.float32) + attn_out).astype(jnp.bfloat16)


def capacity_for(n_tokens, top_k, n_experts):
    return ((5 * n_tokens * top_k) // (4 * n_experts) + 7) // 8 * 8


def nt_dot(lhs, rhs):
    return lax.dot_general(lhs, rhs, (((1,), (1,)), ((), ())), preferred_element_type=jnp.float32)


def solution(mesh):
    n_f, n_ep = mesh.shape["fsdp"], mesh.shape["ep"]
    n_core = 2
    n_x = n_ep // n_core
    phys = Mesh(mesh.devices.reshape(n_f, n_x, n_core), ALL)
    tok_spec = P(ALL)
    row_spec = P("fsdp", None)
    ep = ("x", "core")

    def gather_rows(shard):
        part = shard.shape[0] // n_ep
        mine = lax.axis_index("x") * n_core + lax.axis_index("core")
        piece = lax.dynamic_slice_in_dim(shard, mine * part, part, 0)
        return lax.all_gather(piece, ALL, axis=0, tiled=True)

    def stage_expert(shard):
        core = lax.axis_index("core")
        half = shard.shape[1] // n_core
        keep = lax.dynamic_slice_in_dim(shard, core * half, half, 1)
        give = lax.dynamic_slice_in_dim(shard, (1 - core) * half, half, 1)
        got = lax.ppermute(give, "core", SWAP)
        first = core == 0
        return jnp.concatenate([jnp.where(first, keep, got), jnp.where(first, got, keep)], axis=0)

    def collect_expert(both):
        first = lax.axis_index("core") == 0
        mine = lax.all_to_all(both, "fsdp", 0, 0, tiled=True)
        other = lax.ppermute(mine, "core", SWAP)
        whole = jnp.stack([jnp.where(first, mine, other), jnp.where(first, other, mine)], axis=1)
        return whole.reshape(-1, both.shape[2])

    def local_step(x_in, w_qkv, w_out, w_gate, w_up, w_down, ws_gate, ws_up, ws_down, expert_ids, slot_ids, gate_vals):
        n_batch, seq_len, model_dim = x_in.shape
        n_tokens = n_batch * seq_len
        top_k = expert_ids.shape[-1]
        n_experts = w_gate.shape[0] * n_ep
        capacity = capacity_for(n_tokens, top_k, n_experts)
        part = capacity // n_core
        n_rows = n_experts * capacity
        s_ff = ws_gate.shape[1]

        n_qkv = w_qkv.shape[1]
        attn_full = gather_rows(jnp.concatenate([w_qkv, w_out], axis=1))
        gate_half = stage_expert(w_gate)
        up_half = stage_expert(w_up)
        down_half = stage_expert(jnp.swapaxes(w_down, 1, 2))
        gate_w = collect_expert(gate_half)
        attn_full, up_half, down_half = lax.optimization_barrier((attn_full, up_half, down_half))
        up_w = collect_expert(up_half)
        down_w = collect_expert(down_half)
        shared_full = gather_rows(jnp.concatenate([ws_gate, ws_up, ws_down.T], axis=1))

        ids = expert_ids.reshape(n_tokens, top_k)
        slots = slot_ids.reshape(n_tokens, top_k)
        gates = gate_vals.reshape(n_tokens, top_k)
        kept = slots >= 0
        dest = ((ids % n_f) * n_x + ids // n_f) * n_core + slots // part
        spot = slots % part
        source_tok = jnp.arange(n_tokens * top_k, dtype=jnp.int32) // top_k
        tok_iota = jnp.arange(n_tokens, dtype=jnp.int32)
        n_dev = n_f * n_ep
        first_part = (2 * part // 3 + 7) // 8 * 8
        bounds = ((0, first_part), (first_part, part))
        low = spot < first_part
        row = jnp.where(low, dest * first_part + spot, n_dev * first_part + dest * (part - first_part) + spot - first_part)
        row = jnp.where(kept, row, n_rows).reshape(-1)
        row_source = jnp.full((n_rows,), n_tokens, jnp.int32).at[row].set(source_tok, mode="drop")
        row_gate = jnp.zeros((n_rows,), gates.dtype).at[row].set(gates.reshape(-1), mode="drop")
        spread = (row_source[:, None] == tok_iota[None, :]).astype(jnp.bfloat16)
        merge = jnp.where(row_source[None, :] == tok_iota[:, None], row_gate[None, :], jnp.zeros((), gates.dtype))

        hidden = attention_block(x_in, attn_full[:, :n_qkv], attn_full[:, n_qkv:]).reshape(n_tokens, model_dim)
        normed = rms_norm(hidden)
        received = []
        for lo, hi in bounds:
            sl = slice(n_dev * lo, n_dev * hi)
            buffer = jnp.dot(spread[sl], normed, preferred_element_type=jnp.float32).astype(jnp.bfloat16)
            received.append(lax.all_to_all(buffer.reshape(n_dev, hi - lo, model_dim), ALL, 0, 0, tiled=True))
        routed = None
        for (lo, hi), got in zip(bounds, received):
            sl = slice(n_dev * lo, n_dev * hi)
            rows_in = got.reshape(n_dev * (hi - lo), model_dim)
            gate_act = jnp.dot(rows_in, gate_w, preferred_element_type=jnp.float32)
            up_act = jnp.dot(rows_in, up_w, preferred_element_type=jnp.float32)
            inner = (jax.nn.silu(gate_act) * up_act).astype(jnp.bfloat16)
            expert_out = nt_dot(inner, down_w).astype(jnp.bfloat16)
            back = lax.all_to_all(expert_out.reshape(n_dev, hi - lo, model_dim), ALL, 0, 0, tiled=True)
            term = jnp.dot(merge[:, sl], back.reshape(n_dev * (hi - lo), model_dim), preferred_element_type=jnp.float32)
            routed = term if routed is None else routed + term

        s_gate = jnp.dot(normed, shared_full[:, :s_ff], preferred_element_type=jnp.float32)
        s_up = jnp.dot(normed, shared_full[:, s_ff:2 * s_ff], preferred_element_type=jnp.float32)
        s_inner = (jax.nn.silu(s_gate) * s_up).astype(jnp.bfloat16)
        shared_out = nt_dot(s_inner, shared_full[:, 2 * s_ff:])
        summed = hidden.astype(jnp.float32) + shared_out + routed
        return summed.astype(jnp.bfloat16).reshape(n_batch, seq_len, model_dim)

    return jax.shard_map(local_step, mesh=phys, in_specs=(tok_spec, row_spec, row_spec, P(ep, "fsdp", None), P(ep, "fsdp", None), P(ep, None, "fsdp"), row_spec, row_spec, P(None, "fsdp"), tok_spec, tok_spec, tok_spec), out_specs=tok_spec, check_vma=False)
```

```python
import functools

import jax
import jax.numpy as jnp
from jax import lax
from jax.experimental import pallas as pl
from jax.experimental.pallas import tpu as pltpu
from jax.sharding import Mesh, PartitionSpec as P


HEAD_DIM = 128
ROPE_BASE = 10000.0
EPSILON = 1e-6
ALL = ("fsdp", "x", "core")
SWAP = [(0, 1), (1, 0)]


def rms_norm(values):
    vals_f32 = values.astype(jnp.float32)
    mean_sq = jnp.mean(vals_f32 * vals_f32, axis=-1, keepdims=True)
    return (vals_f32 * lax.rsqrt(mean_sq + EPSILON)).astype(jnp.bfloat16)


def rotary_embed(heads_in, positions):
    half_dim = HEAD_DIM // 2
    inv_freq = ROPE_BASE ** (-jnp.arange(half_dim, dtype=jnp.float32) * (2.0 / HEAD_DIM))
    angles = positions[:, None] * inv_freq[None, :]
    cos_tab = jnp.cos(angles)[:, None, :]
    sin_tab = jnp.sin(angles)[:, None, :]
    vals_f32 = heads_in.astype(jnp.float32)
    first_half = vals_f32[..., :half_dim]
    second_half = vals_f32[..., half_dim:]
    rotated = jnp.concatenate([first_half * cos_tab - second_half * sin_tab, second_half * cos_tab + first_half * sin_tab], axis=-1)
    return rotated.astype(jnp.bfloat16)


def attention_block(x_in, qkv_weight, out_weight):
    n_batch, seq_len, _ = x_in.shape
    n_heads = qkv_weight.shape[1] // (3 * HEAD_DIM)
    normed = rms_norm(x_in)
    qkv_proj = jnp.einsum("bsd,dn->bsn", normed, qkv_weight, preferred_element_type=jnp.float32).astype(jnp.bfloat16)
    qkv_proj = qkv_proj.reshape(n_batch, seq_len, 3, n_heads, HEAD_DIM)
    positions = jnp.arange(seq_len, dtype=jnp.float32)
    query_rot = rotary_embed(qkv_proj[:, :, 0], positions)
    key_rot = rotary_embed(qkv_proj[:, :, 1], positions)
    scores = jnp.einsum("bqhd,bkhd->bhqk", query_rot, key_rot, preferred_element_type=jnp.float32) * (HEAD_DIM ** -0.5)
    causal = jnp.arange(seq_len)[:, None] >= jnp.arange(seq_len)[None, :]
    attn_probs = jax.nn.softmax(jnp.where(causal, scores, -1e30), axis=-1).astype(jnp.bfloat16)
    attn_mixed = jnp.einsum("bhqk,bkhd->bqhd", attn_probs, qkv_proj[:, :, 2], preferred_element_type=jnp.float32).astype(jnp.bfloat16)
    attn_out = jnp.einsum("bsn,nm->bsm", attn_mixed.reshape(n_batch, seq_len, n_heads * HEAD_DIM), out_weight, preferred_element_type=jnp.float32)
    return (x_in.astype(jnp.float32) + attn_out).astype(jnp.bfloat16)


def capacity_for(n_tokens, top_k, n_experts):
    return ((5 * n_tokens * top_k) // (4 * n_experts) + 7) // 8 * 8


def nt_dot(lhs, rhs):
    return lax.dot_general(lhs, rhs, (((1,), (1,)), ((), ())), preferred_element_type=jnp.float32)


def exchange_kernel(n_chunk, inp, half, out, r1, r2, r3, b1, b2, own, w13, w2, xin, inner, yall, w_sem, in_sem, tx, rx, fin, ld):
    f, x, core = lax.axis_index("fsdp"), lax.axis_index("x"), lax.axis_index("core")
    z, y = f // 4, f % 4
    copy = pltpu.make_async_copy

    def dev(dx=0, dz=0, dy=0, dc=0):
        return {"fsdp": (z + dz + 4) % 4 * 4 + (y + dy + 4) % 4, "x": (x + dx + 4) % 4, "core": (core + dc) % 2}

    def send(src, dst, ssem, rsem, to):
        pltpu.make_async_remote_copy(src_ref=src, dst_ref=dst, send_sem=ssem, recv_sem=rsem, device_id=to, device_id_type=pl.DeviceIdType.MESH).start()

    def wait(ref, sem):
        copy(ref, ref, sem).wait()

    for k in range(n_chunk):
        for a in (1, 3, 2):
            send(inp.at[k, a], r1.at[k, a - 1], tx.at[0], rx.at[0, k], dev(dx=a))

    n_tile = half.shape[2] // 384
    for part in range(2):
        for j in range(n_tile):
            src = half.at[:, :, pl.ds((part * n_tile + j) * 128, 128)]
            dst = w13.at[:, core, :, pl.ds(j * 256 + part * 128, 128)]
            copy(src, dst, w_sem.at[0]).start()
            send(src, dst, w_sem.at[2], w_sem.at[4], dev(dc=1))
    down_h = half.at[:, :, pl.ds(n_tile * 256, n_tile * 128)]
    copy(down_h, w2.at[:, core], w_sem.at[1]).start()
    send(down_h, w2.at[:, core], w_sem.at[3], w_sem.at[5], dev(dc=1))

    def step(t, carry):
        @pl.when(t < n_chunk)
        def _():
            k = t
            wait(r1.at[k], rx.at[0, k])
            for b in (1, 3, 2):
                send(r1.at[k, :, b], r2.at[k, b - 1, pl.ds(1, 3)], tx.at[1], rx.at[1, k], dev(dz=b))
                send(inp.at[k, 0, b], r2.at[k, b - 1, 0], tx.at[1], rx.at[1, k], dev(dz=b))

        @pl.when((t >= 1) & (t < n_chunk + 1))
        def _():
            k = t - 1
            wait(r2.at[k], rx.at[1, k])
            for c in (1, 3, 2):
                send(r2.at[k, :, :, c], r3.at[k, c - 1, pl.ds(1, 3)], tx.at[2], rx.at[2, k], dev(dy=c))
                send(r1.at[k, :, 0, c], r3.at[k, c - 1, 0, pl.ds(1, 3)], tx.at[2], rx.at[2, k], dev(dy=c))
                send(inp.at[k, 0, 0, c], r3.at[k, c - 1, 0, 0], tx.at[2], rx.at[2, k], dev(dy=c))

        @pl.when((t >= 4) & (t < n_chunk + 4))
        def _():
            k = t - 4
            wait(b1.at[k], rx.at[3, k])
            for b in (1, 3, 2):
                to = dev(dz=-b)
                send(b1.at[k, :, b, pl.ds(1, 3)], b2.at[k, b - 1, pl.ds(1, 3)], tx.at[4], rx.at[4, k], to)
                send(own.at[k, b, pl.ds(1, 3)], b2.at[k, b - 1, 0], tx.at[4], rx.at[4, k], to)
                send(b1.at[k, :, b, 0], out.at[k, 0, b, pl.ds(1, 3)], tx.at[5], fin.at[1], to)
                send(own.at[k, b, 0], out.at[k, 0, b, 0], tx.at[5], fin.at[1], to)

        @pl.when((t >= 5) & (t < n_chunk + 5))
        def _():
            k = t - 5
            wait(b2.at[k], rx.at[4, k])
            for a in (1, 3, 2):
                to = dev(dx=-a)
                send(b2.at[k, :, :, a - 1], out.at[k, a, pl.ds(1, 3)], tx.at[6], fin.at[0], to)
                send(b1.at[k, :, 0, a], out.at[k, a, 0, pl.ds(1, 3)], tx.at[6], fin.at[0], to)
                send(own.at[k, 0, a], out.at[k, a, 0, 0], tx.at[6], fin.at[0], to)

        @pl.when((t >= 2) & (t < n_chunk + 2))
        def _():
            k = t - 2
            wait(r3.at[k], rx.at[2, k])

            @pl.when(t == 2)
            def _():
                for i in (0, 2, 4):
                    wait(w13.at[:, 0], w_sem.at[i])
                for i in (1, 3, 5):
                    wait(w2.at[:, 0], w_sem.at[i])

            copy(r3.at[k], xin.at[pl.ds(1, 3)], in_sem).start()
            copy(r2.at[k, :, :, 0], xin.at[0, pl.ds(1, 3)], in_sem).start()
            copy(r1.at[k, :, 0, 0], xin.at[0, 0, pl.ds(1, 3)], in_sem).start()
            copy(inp.at[k, 0, 0, 0], xin.at[0, 0, 0], in_sem).start()
            wait(xin, in_sem)
            rows = xin.shape[0] * xin.shape[1] * xin.shape[2] * xin.shape[3]

            def up_tile(j, c2):
                lhs = xin[...].reshape(rows, xin.shape[4])
                cols = w13[:, :, :, pl.ds(pl.multiple_of(j * 256, 256), 256)].reshape(-1, 256)
                both = jnp.dot(lhs, cols, preferred_element_type=jnp.float32)
                act = jax.nn.silu(both[:, :128]) * both[:, 128:]
                inner[:, pl.ds(pl.multiple_of(j * 128, 128), 128)] = act.astype(jnp.bfloat16)
                return c2

            lax.fori_loop(0, n_tile, up_tile, 0)

            def down_tile(n, c2):
                rhs = w2[pl.ds(n * 2, 2)].reshape(256, w2.shape[3])
                res = lax.dot_general(inner[...], rhs, (((1,), (1,)), ((), ())), preferred_element_type=jnp.float32)
                yall[k, :, :, :, :, pl.ds(pl.multiple_of(n * 256, 256), 256)] = res.astype(jnp.bfloat16).reshape(4, 4, 4, 8, 256)
                return c2

            lax.fori_loop(0, w2.shape[0] // 2, down_tile, 0)
            copy(yall.at[k, 0], own.at[k], ld.at[0]).start()
            copy(yall.at[k, 0, 0, 0], out.at[k, 0, 0, 0], ld.at[1]).start()
            for c in (1, 3, 2):
                send(yall.at[k, c], b1.at[k, c - 1], tx.at[3], rx.at[3, k], dev(dy=-c))
                send(yall.at[k, c, 0, 0], out.at[k, 0, 0, c], tx.at[7], fin.at[2], dev(dy=-c))
            wait(own.at[k], ld.at[0])
            wait(out.at[k, 0, 0, 0], ld.at[1])

        return carry

    lax.fori_loop(0, n_chunk + 5, step, 0)
    wait(out.at[:, pl.ds(1, 3)], tx.at[6])
    wait(out.at[:, 0, pl.ds(1, 3)], tx.at[5])
    wait(out.at[:, 0, 0, pl.ds(1, 3)], tx.at[7])
    for ref, i in ((r1, 0), (r2, 1), (r3, 2), (b1, 3), (b2, 4)):
        wait(ref, tx.at[i])
    wait(out.at[:, pl.ds(1, 3)], fin.at[0])
    wait(out.at[:, 0, pl.ds(1, 3)], fin.at[1])
    wait(out.at[:, 0, 0, pl.ds(1, 3)], fin.at[2])


def run_exchange(inp, half):
    n_chunk, _, _, _, blk, dim = inp.shape
    width = half.shape[2] // 3
    bf = jnp.bfloat16
    shapes = [(4, 4, 4), (3, 4, 4), (3, 4, 4), (3, 4, 4), (3, 4, 4), (3, 4, 3), (4, 4)]
    outs = pl.pallas_call(
        functools.partial(exchange_kernel, n_chunk),
        out_shape=[jax.ShapeDtypeStruct((n_chunk,) + sh + (blk, dim), bf) for sh in shapes],
        in_specs=[pl.BlockSpec(memory_space=pl.ANY)] * 2,
        out_specs=[pl.BlockSpec(memory_space=pl.ANY)] * len(shapes),
        scratch_shapes=[
            pltpu.VMEM((16, 2, 64, 2 * width), bf),
            pltpu.VMEM((16, 2, 64, width), bf),
            pltpu.VMEM((4, 4, 4, blk, dim), bf),
            pltpu.VMEM((64 * blk, width), bf),
            pltpu.VMEM((n_chunk, 4, 4, 4, blk, dim), bf),
            pltpu.SemaphoreType.DMA((6,)),
            pltpu.SemaphoreType.DMA,
            pltpu.SemaphoreType.DMA((8,)),
            pltpu.SemaphoreType.DMA((5, n_chunk)),
            pltpu.SemaphoreType.DMA((3,)),
            pltpu.SemaphoreType.DMA((2,)),
        ],
        compiler_params=pltpu.CompilerParams(has_side_effects=True, vmem_limit_bytes=60 * 2**20),
        name="expert_exchange",
    )(inp, half)
    return outs[0]


def solution(mesh):
    n_f, n_ep = mesh.shape["fsdp"], mesh.shape["ep"]
    n_core = 2
    n_x = n_ep // n_core
    phys = Mesh(mesh.devices.reshape(n_f, n_x, n_core), ALL)
    tok_spec = P(ALL)
    row_spec = P("fsdp", None)
    ep = ("x", "core")

    def gather_rows(*shards):
        part = shards[0].shape[0] // n_ep
        mine = lax.axis_index("x") * n_core + lax.axis_index("core")
        piece = jnp.concatenate([lax.dynamic_slice_in_dim(shard, mine * part, part, 0) for shard in shards], axis=1)
        return lax.all_gather(piece, ALL, axis=0, tiled=True)

    def stage_expert(shard):
        core = lax.axis_index("core")
        half = shard.shape[1] // n_core
        keep = lax.dynamic_slice_in_dim(shard, core * half, half, 1)
        give = lax.dynamic_slice_in_dim(shard, (1 - core) * half, half, 1)
        got = lax.ppermute(give, "core", SWAP)
        first = core == 0
        return jnp.concatenate([jnp.where(first, keep, got), jnp.where(first, got, keep)], axis=0)

    def local_step(x_in, w_qkv, w_out, w_gate, w_up, w_down, ws_gate, ws_up, ws_down, expert_ids, slot_ids, gate_vals):
        n_batch, seq_len, model_dim = x_in.shape
        n_tokens = n_batch * seq_len
        top_k = expert_ids.shape[-1]
        n_experts = w_gate.shape[0] * n_ep
        capacity = capacity_for(n_tokens, top_k, n_experts)
        n_rows = n_experts * capacity
        s_ff = ws_gate.shape[1]

        n_qkv = w_qkv.shape[1]
        n_attn = n_qkv + w_out.shape[1]
        dense = gather_rows(w_qkv, w_out, ws_gate, ws_up, lax.optimization_barrier(ws_down.T))
        half = jnp.concatenate([stage_expert(w_gate), stage_expert(w_up), stage_expert(jnp.swapaxes(w_down, 1, 2))], axis=2)
        dense, half = lax.optimization_barrier((dense, half))
        half = lax.all_to_all(half, "fsdp", 0, 0, tiled=True)
        qkv_full, out_full, shared_full = dense[:, :n_qkv], dense[:, n_qkv:n_attn], dense[:, n_attn:]

        ids = expert_ids.reshape(n_tokens, top_k)
        slots = slot_ids.reshape(n_tokens, top_k)
        gates = gate_vals.reshape(n_tokens, top_k)
        kept = slots >= 0
        far, chip = lax.axis_index("fsdp"), lax.axis_index("x")
        rel_x = (ids // n_f - chip) % 4
        rel_z = (ids % n_f // 4 - far // 4) % 4
        rel_y = (ids % 4 - far % 4) % 4
        n_chunk = capacity // 8
        row = ((slots // 8 * 4 + rel_x) * 4 + rel_z) * 4 + rel_y
        row = jnp.where(kept, row * 8 + slots % 8, n_rows).reshape(-1)
        source_tok = jnp.arange(n_tokens * top_k, dtype=jnp.int32) // top_k
        tok_iota = jnp.arange(n_tokens, dtype=jnp.int32)
        row_source = jnp.full((n_rows,), n_tokens, jnp.int32).at[row].set(source_tok, mode="drop")
        row_gate = jnp.zeros((n_rows,), gates.dtype).at[row].set(gates.reshape(-1), mode="drop")
        spread = (row_source[:, None] == tok_iota[None, :]).astype(jnp.bfloat16)
        merge = jnp.where(row_source[None, :] == tok_iota[:, None], row_gate[None, :], jnp.zeros((), gates.dtype))

        hidden = attention_block(x_in, qkv_full, out_full).reshape(n_tokens, model_dim)
        normed = rms_norm(hidden)
        buffer = jnp.dot(spread, normed, preferred_element_type=jnp.float32).astype(jnp.bfloat16)
        s_gate = jnp.dot(normed, shared_full[:, :s_ff], preferred_element_type=jnp.float32)
        s_up = jnp.dot(normed, shared_full[:, s_ff:2 * s_ff], preferred_element_type=jnp.float32)
        s_inner = (jax.nn.silu(s_gate) * s_up).astype(jnp.bfloat16)
        shared_out = nt_dot(s_inner, shared_full[:, 2 * s_ff:])
        buffer, shared_out = lax.optimization_barrier((buffer, shared_out))
        back = run_exchange(buffer.reshape(n_chunk, 4, 4, 4, 8, model_dim), half)
        routed = jnp.dot(merge, back.reshape(n_rows, model_dim), preferred_element_type=jnp.float32)

        summed = hidden.astype(jnp.float32) + shared_out + routed
        return summed.astype(jnp.bfloat16).reshape(n_batch, seq_len, model_dim)

    return jax.shard_map(local_step, mesh=phys, in_specs=(tok_spec, row_spec, row_spec, P(ep, "fsdp", None), P(ep, "fsdp", None), P(ep, None, "fsdp"), row_spec, row_spec, P(None, "fsdp"), tok_spec, tok_spec, tok_spec), out_specs=tok_spec, check_vma=False)
```

```python
import functools

import jax
import jax.numpy as jnp
from jax import lax
from jax.experimental import pallas as pl
from jax.experimental.pallas import tpu as pltpu
from jax.sharding import Mesh, PartitionSpec as P


HEAD_DIM = 128
ROPE_BASE = 10000.0
EPSILON = 1e-6
ALL = ("fsdp", "x", "core")
SWAP = [(0, 1), (1, 0)]


def rms_norm(values):
    vals_f32 = values.astype(jnp.float32)
    mean_sq = jnp.mean(vals_f32 * vals_f32, axis=-1, keepdims=True)
    return (vals_f32 * lax.rsqrt(mean_sq + EPSILON)).astype(jnp.bfloat16)


def rotary_embed(heads_in, positions):
    half_dim = HEAD_DIM // 2
    inv_freq = ROPE_BASE ** (-jnp.arange(half_dim, dtype=jnp.float32) * (2.0 / HEAD_DIM))
    angles = positions[:, None] * inv_freq[None, :]
    cos_tab = jnp.cos(angles)[:, None, :]
    sin_tab = jnp.sin(angles)[:, None, :]
    vals_f32 = heads_in.astype(jnp.float32)
    first_half = vals_f32[..., :half_dim]
    second_half = vals_f32[..., half_dim:]
    rotated = jnp.concatenate([first_half * cos_tab - second_half * sin_tab, second_half * cos_tab + first_half * sin_tab], axis=-1)
    return rotated.astype(jnp.bfloat16)


def attention_block(x_in, qkv_weight, out_weight):
    n_batch, seq_len, _ = x_in.shape
    n_heads = qkv_weight.shape[1] // (3 * HEAD_DIM)
    normed = rms_norm(x_in)
    qkv_proj = jnp.einsum("bsd,dn->bsn", normed, qkv_weight, preferred_element_type=jnp.float32).astype(jnp.bfloat16)
    qkv_proj = qkv_proj.reshape(n_batch, seq_len, 3, n_heads, HEAD_DIM)
    positions = jnp.arange(seq_len, dtype=jnp.float32)
    query_rot = rotary_embed(qkv_proj[:, :, 0], positions)
    key_rot = rotary_embed(qkv_proj[:, :, 1], positions)
    scores = jnp.einsum("bqhd,bkhd->bhqk", query_rot, key_rot, preferred_element_type=jnp.float32) * (HEAD_DIM ** -0.5)
    causal = jnp.arange(seq_len)[:, None] >= jnp.arange(seq_len)[None, :]
    attn_probs = jax.nn.softmax(jnp.where(causal, scores, -1e30), axis=-1).astype(jnp.bfloat16)
    attn_mixed = jnp.einsum("bhqk,bkhd->bqhd", attn_probs, qkv_proj[:, :, 2], preferred_element_type=jnp.float32).astype(jnp.bfloat16)
    attn_out = jnp.einsum("bsn,nm->bsm", attn_mixed.reshape(n_batch, seq_len, n_heads * HEAD_DIM), out_weight, preferred_element_type=jnp.float32)
    return (x_in.astype(jnp.float32) + attn_out).astype(jnp.bfloat16)


def capacity_for(n_tokens, top_k, n_experts):
    return ((5 * n_tokens * top_k) // (4 * n_experts) + 7) // 8 * 8


def nt_dot(lhs, rhs):
    return lax.dot_general(lhs, rhs, (((1,), (1,)), ((), ())), preferred_element_type=jnp.float32)


def exchange_kernel(n_chunk, inp, gate_h, rest_h, out, r1, r2, r3, b1, b2, own, w13, w2, xin, inner, yall, w_sem, in_sem, tx, rx, fin, ld):
    f, x, core = lax.axis_index("fsdp"), lax.axis_index("x"), lax.axis_index("core")
    z, y = f // 4, f % 4
    copy = pltpu.make_async_copy

    def dev(axis, hop):
        d = [0, 0, 0]
        d[axis % 3] = hop + 4
        return {"fsdp": (z + d[1]) % 4 * 4 + (y + d[2]) % 4, "x": (x + d[0]) % 4, "core": core}

    def send(src, dst, ssem, rsem, to):
        pltpu.make_async_remote_copy(src_ref=src, dst_ref=dst, send_sem=ssem, recv_sem=rsem, device_id=to, device_id_type=pl.DeviceIdType.MESH).start()

    def wait(ref, sem):
        copy(ref, ref, sem).wait()

    def hop1(k):
        for h in (1, 3, 2):
            send(inp.at[k, h], r1.at[k, h - 1], tx.at[0], rx.at[0, k], dev(k, h))

    def hop2(k):
        wait(r1.at[k], rx.at[0, k])
        for h in (1, 3, 2):
            to = dev(k + 1, h)
            send(r1.at[k, :, h], r2.at[k, h - 1, pl.ds(1, 3)], tx.at[1], rx.at[1, k], to)
            send(inp.at[k, 0, h], r2.at[k, h - 1, 0], tx.at[1], rx.at[1, k], to)

    def hop3(k):
        wait(r2.at[k], rx.at[1, k])
        for h in (1, 3, 2):
            to = dev(k + 2, h)
            send(r2.at[k, :, :, h], r3.at[k, h - 1, pl.ds(1, 3)], tx.at[2], rx.at[2, k], to)
            send(r1.at[k, :, 0, h], r3.at[k, h - 1, 0, pl.ds(1, 3)], tx.at[2], rx.at[2, k], to)
            send(inp.at[k, 0, 0, h], r3.at[k, h - 1, 0, 0], tx.at[2], rx.at[2, k], to)

    def back2(k):
        wait(b1.at[k], rx.at[3, k])
        for h in (1, 3, 2):
            to = dev(k + 1, -h)
            send(b1.at[k, :, h, pl.ds(1, 3)], b2.at[k, h - 1, pl.ds(1, 3)], tx.at[4], rx.at[4, k], to)
            send(own.at[k, h, pl.ds(1, 3)], b2.at[k, h - 1, 0], tx.at[4], rx.at[4, k], to)
            send(b1.at[k, :, h, 0], out.at[k, 0, h, pl.ds(1, 3)], tx.at[5], fin.at[1], to)
            send(own.at[k, h, 0], out.at[k, 0, h, 0], tx.at[5], fin.at[1], to)

    def back3(k):
        wait(b2.at[k], rx.at[4, k])
        for h in (1, 3, 2):
            to = dev(k, -h)
            send(b2.at[k, :, :, h - 1], out.at[k, h, pl.ds(1, 3)], tx.at[6], fin.at[0], to)
            send(b1.at[k, :, 0, h], out.at[k, h, 0, pl.ds(1, 3)], tx.at[6], fin.at[0], to)
            send(own.at[k, 0, h], out.at[k, h, 0, 0], tx.at[6], fin.at[0], to)

    def load(k):
        wait(r3.at[k], rx.at[2, k])
        copy(r3.at[k], xin.at[pl.ds(1, 3)], in_sem).start()
        copy(r2.at[k, :, :, 0], xin.at[0, pl.ds(1, 3)], in_sem).start()
        copy(r1.at[k, :, 0, 0], xin.at[0, 0, pl.ds(1, 3)], in_sem).start()
        copy(inp.at[k, 0, 0, 0], xin.at[0, 0, 0], in_sem).start()
        wait(xin, in_sem)

    n_tile = gate_h.shape[2] // 128

    def experts(k):
        load(k)
        rows = xin.shape[0] * xin.shape[1] * xin.shape[2] * xin.shape[3]

        def up_tile(j, carry):
            lhs = xin[...].reshape(rows, xin.shape[4])
            cols = w13[:, :, :, pl.ds(pl.multiple_of(j * 256, 256), 256)].reshape(-1, 256)
            both = jnp.dot(lhs, cols, preferred_element_type=jnp.float32)
            act = jax.nn.silu(both[:, :128]) * both[:, 128:]
            inner[:, pl.ds(pl.multiple_of(j * 128, 128), 128)] = act.astype(jnp.bfloat16)
            return carry

        lax.fori_loop(0, n_tile, up_tile, 0)

        def down_tile(n, carry):
            rhs = w2[pl.ds(n * 2, 2)].reshape(256, w2.shape[3])
            res = lax.dot_general(inner[...], rhs, (((1,), (1,)), ((), ())), preferred_element_type=jnp.float32)
            yall[k, :, :, :, :, pl.ds(pl.multiple_of(n * 256, 256), 256)] = res.astype(jnp.bfloat16).reshape(4, 4, 4, 8, 256)
            return carry

        lax.fori_loop(0, w2.shape[0] // 2, down_tile, 0)

    def back1(k):
        copy(yall.at[k, 0], own.at[k], ld.at[0, k]).start()
        copy(yall.at[k, 0, 0, 0], out.at[k, 0, 0, 0], ld.at[1, k]).start()
        for h in (1, 3, 2):
            to = dev(k + 2, -h)
            send(yall.at[k, h], b1.at[k, h - 1], tx.at[3], rx.at[3, k], to)
            send(yall.at[k, h, 0, 0], out.at[k, 0, 0, h], tx.at[7], fin.at[2], to)

    def landed(k):
        wait(own.at[k], ld.at[0, k])
        wait(out.at[k, 0, 0, 0], ld.at[1, k])

    early, late = range(0, n_chunk // 2), range(n_chunk // 2, n_chunk)
    for k in early:
        hop1(k)
    partner = {"core": 1 - core}
    for part, (half, base) in enumerate(((gate_h, 0), (rest_h, 0))):
        for j in range(n_tile):
            src = half.at[:, :, pl.ds(base + j * 128, 128)]
            dst = w13.at[:, core, :, pl.ds(j * 256 + part * 128, 128)]
            copy(src, dst, w_sem.at[0]).start()
            send(src, dst, w_sem.at[2], w_sem.at[4], partner)
    down_h = rest_h.at[:, :, pl.ds(n_tile * 128, n_tile * 128)]
    copy(down_h, w2.at[:, core], w_sem.at[1]).start()
    send(down_h, w2.at[:, core], w_sem.at[3], w_sem.at[5], partner)

    for k in early:
        hop2(k)
    for k in late:
        hop1(k)
    for k in early:
        hop3(k)
    for k in late:
        hop2(k)
    for i in (0, 2, 4):
        wait(w13.at[:, 0], w_sem.at[i])
    for i in (1, 3, 5):
        wait(w2.at[:, 0], w_sem.at[i])
    for i, k in enumerate(early):
        experts(k)
        back1(k)
        if i == 0:
            for q in late:
                hop3(q)
    for k in early:
        landed(k)
        back2(k)
    for i, k in enumerate(late):
        experts(k)
        back1(k)
        if i == 1:
            for q in early:
                back3(q)
    for k in late:
        landed(k)
        back2(k)
    for k in late:
        back3(k)

    wait(out.at[:, pl.ds(1, 3)], tx.at[6])
    wait(out.at[:, 0, pl.ds(1, 3)], tx.at[5])
    wait(out.at[:, 0, 0, pl.ds(1, 3)], tx.at[7])
    for ref, i in ((r1, 0), (r2, 1), (r3, 2), (b1, 3), (b2, 4)):
        wait(ref, tx.at[i])
    wait(out.at[:, pl.ds(1, 3)], fin.at[0])
    wait(out.at[:, 0, pl.ds(1, 3)], fin.at[1])
    wait(out.at[:, 0, 0, pl.ds(1, 3)], fin.at[2])


def run_exchange(inp, gate_h, rest_h):
    n_chunk, _, _, _, blk, dim = inp.shape
    width = gate_h.shape[2]
    bf = jnp.bfloat16
    shapes = [(4, 4, 4), (3, 4, 4), (3, 4, 4), (3, 4, 4), (3, 4, 4), (3, 4, 3), (4, 4)]
    outs = pl.pallas_call(
        functools.partial(exchange_kernel, n_chunk),
        out_shape=[jax.ShapeDtypeStruct((n_chunk,) + sh + (blk, dim), bf) for sh in shapes],
        in_specs=[pl.BlockSpec(memory_space=pl.ANY)] * 3,
        out_specs=[pl.BlockSpec(memory_space=pl.ANY)] * len(shapes),
        scratch_shapes=[
            pltpu.VMEM((16, 2, 64, 2 * width), bf),
            pltpu.VMEM((16, 2, 64, width), bf),
            pltpu.VMEM((4, 4, 4, blk, dim), bf),
            pltpu.VMEM((64 * blk, width), bf),
            pltpu.VMEM((n_chunk, 4, 4, 4, blk, dim), bf),
            pltpu.SemaphoreType.DMA((6,)),
            pltpu.SemaphoreType.DMA,
            pltpu.SemaphoreType.DMA((8,)),
            pltpu.SemaphoreType.DMA((5, n_chunk)),
            pltpu.SemaphoreType.DMA((3,)),
            pltpu.SemaphoreType.DMA((2, n_chunk)),
        ],
        compiler_params=pltpu.CompilerParams(has_side_effects=True, vmem_limit_bytes=60 * 2**20),
        name="expert_exchange",
    )(inp, gate_h, rest_h)
    return outs[0]


def solution(mesh):
    n_f, n_ep = mesh.shape["fsdp"], mesh.shape["ep"]
    n_core = 2
    n_x = n_ep // n_core
    phys = Mesh(mesh.devices.reshape(n_f, n_x, n_core), ALL)
    tok_spec = P(ALL)
    row_spec = P("fsdp", None)
    ep = ("x", "core")

    def gather_rows(*shards):
        part = shards[0].shape[0] // n_ep
        mine = lax.axis_index("x") * n_core + lax.axis_index("core")
        piece = jnp.concatenate([lax.dynamic_slice_in_dim(shard, mine * part, part, 0) for shard in shards], axis=1)
        return lax.all_gather(piece, ALL, axis=0, tiled=True)

    def stage_expert(shard):
        core = lax.axis_index("core")
        half = shard.shape[1] // n_core
        keep = lax.dynamic_slice_in_dim(shard, core * half, half, 1)
        give = lax.dynamic_slice_in_dim(shard, (1 - core) * half, half, 1)
        got = lax.ppermute(give, "core", SWAP)
        first = core == 0
        return jnp.concatenate([jnp.where(first, keep, got), jnp.where(first, got, keep)], axis=0)

    def local_step(x_in, w_qkv, w_out, w_gate, w_up, w_down, ws_gate, ws_up, ws_down, expert_ids, slot_ids, gate_vals):
        n_batch, seq_len, model_dim = x_in.shape
        n_tokens = n_batch * seq_len
        top_k = expert_ids.shape[-1]
        n_experts = w_gate.shape[0] * n_ep
        capacity = capacity_for(n_tokens, top_k, n_experts)
        n_rows = n_experts * capacity
        s_ff = ws_gate.shape[1]

        n_qkv = w_qkv.shape[1]
        n_attn = n_qkv + w_out.shape[1]
        dense = gather_rows(w_qkv, w_out, ws_gate, ws_up, lax.optimization_barrier(ws_down.T))
        gate_h = lax.all_to_all(stage_expert(w_gate), "fsdp", 0, 0, tiled=True)
        rest = jnp.concatenate([stage_expert(w_up), stage_expert(jnp.swapaxes(w_down, 1, 2))], axis=2)
        dense, rest, gate_h = lax.optimization_barrier((dense, rest, gate_h))
        rest_h = lax.all_to_all(rest, "fsdp", 0, 0, tiled=True)
        qkv_full, out_full, shared_full = dense[:, :n_qkv], dense[:, n_qkv:n_attn], dense[:, n_attn:]

        ids = expert_ids.reshape(n_tokens, top_k)
        slots = slot_ids.reshape(n_tokens, top_k)
        gates = gate_vals.reshape(n_tokens, top_k)
        kept = slots >= 0
        far, chip = lax.axis_index("fsdp"), lax.axis_index("x")
        rel_x = (ids // n_f - chip) % 4
        rel_z = (ids % n_f // 4 - far // 4) % 4
        rel_y = (ids % 4 - far % 4) % 4
        n_chunk = capacity // 8
        turn = slots // 8 % 3
        hop_a = jnp.where(turn == 0, rel_x, jnp.where(turn == 1, rel_z, rel_y))
        hop_b = jnp.where(turn == 0, rel_z, jnp.where(turn == 1, rel_y, rel_x))
        hop_c = jnp.where(turn == 0, rel_y, jnp.where(turn == 1, rel_x, rel_z))
        row = ((slots // 8 * 4 + hop_a) * 4 + hop_b) * 4 + hop_c
        row = jnp.where(kept, row * 8 + slots % 8, n_rows).reshape(-1)
        source_tok = jnp.arange(n_tokens * top_k, dtype=jnp.int32) // top_k
        tok_iota = jnp.arange(n_tokens, dtype=jnp.int32)
        row_source = jnp.full((n_rows,), n_tokens, jnp.int32).at[row].set(source_tok, mode="drop")
        row_gate = jnp.zeros((n_rows,), gates.dtype).at[row].set(gates.reshape(-1), mode="drop")
        spread = (row_source[:, None] == tok_iota[None, :]).astype(jnp.bfloat16)
        merge = jnp.where(row_source[None, :] == tok_iota[:, None], row_gate[None, :], jnp.zeros((), gates.dtype))

        hidden = attention_block(x_in, qkv_full, out_full).reshape(n_tokens, model_dim)
        normed = rms_norm(hidden)
        buffer = jnp.dot(spread, normed, preferred_element_type=jnp.float32).astype(jnp.bfloat16)
        s_gate = jnp.dot(normed, shared_full[:, :s_ff], preferred_element_type=jnp.float32)
        s_up = jnp.dot(normed, shared_full[:, s_ff:2 * s_ff], preferred_element_type=jnp.float32)
        s_inner = (jax.nn.silu(s_gate) * s_up).astype(jnp.bfloat16)
        shared_out = nt_dot(s_inner, shared_full[:, 2 * s_ff:])
        buffer, shared_out = lax.optimization_barrier((buffer, shared_out))
        back = run_exchange(buffer.reshape(n_chunk, 4, 4, 4, 8, model_dim), gate_h, rest_h)
        routed = jnp.dot(merge, back.reshape(n_rows, model_dim), preferred_element_type=jnp.float32)

        summed = hidden.astype(jnp.float32) + shared_out + routed
        return summed.astype(jnp.bfloat16).reshape(n_batch, seq_len, model_dim)

    return jax.shard_map(local_step, mesh=phys, in_specs=(tok_spec, row_spec, row_spec, P(ep, "fsdp", None), P(ep, "fsdp", None), P(ep, None, "fsdp"), row_spec, row_spec, P(None, "fsdp"), tok_spec, tok_spec, tok_spec), out_specs=tok_spec, check_vma=False)
```

```python
import functools

import jax
import jax.numpy as jnp
from jax import lax
from jax.experimental import pallas as pl
from jax.experimental.pallas import tpu as pltpu
from jax.sharding import Mesh, PartitionSpec as P


HEAD_DIM = 128
ROPE_BASE = 10000.0
EPSILON = 1e-6
ALL = ("fsdp", "x", "core")
SWAP = [(0, 1), (1, 0)]


def rms_norm(values):
    vals_f32 = values.astype(jnp.float32)
    mean_sq = jnp.mean(vals_f32 * vals_f32, axis=-1, keepdims=True)
    return (vals_f32 * lax.rsqrt(mean_sq + EPSILON)).astype(jnp.bfloat16)


def rotary_embed(heads_in, positions):
    half_dim = HEAD_DIM // 2
    inv_freq = ROPE_BASE ** (-jnp.arange(half_dim, dtype=jnp.float32) * (2.0 / HEAD_DIM))
    angles = positions[:, None] * inv_freq[None, :]
    cos_tab = jnp.cos(angles)[:, None, :]
    sin_tab = jnp.sin(angles)[:, None, :]
    vals_f32 = heads_in.astype(jnp.float32)
    first_half = vals_f32[..., :half_dim]
    second_half = vals_f32[..., half_dim:]
    rotated = jnp.concatenate([first_half * cos_tab - second_half * sin_tab, second_half * cos_tab + first_half * sin_tab], axis=-1)
    return rotated.astype(jnp.bfloat16)


def attention_block(x_in, qkv_weight, out_weight):
    n_batch, seq_len, _ = x_in.shape
    n_heads = qkv_weight.shape[1] // (3 * HEAD_DIM)
    normed = rms_norm(x_in)
    qkv_proj = jnp.einsum("bsd,dn->bsn", normed, qkv_weight, preferred_element_type=jnp.float32).astype(jnp.bfloat16)
    qkv_proj = qkv_proj.reshape(n_batch, seq_len, 3, n_heads, HEAD_DIM)
    positions = jnp.arange(seq_len, dtype=jnp.float32)
    query_rot = rotary_embed(qkv_proj[:, :, 0], positions)
    key_rot = rotary_embed(qkv_proj[:, :, 1], positions)
    scores = jnp.einsum("bqhd,bkhd->bhqk", query_rot, key_rot, preferred_element_type=jnp.float32) * (HEAD_DIM ** -0.5)
    causal = jnp.arange(seq_len)[:, None] >= jnp.arange(seq_len)[None, :]
    attn_probs = jax.nn.softmax(jnp.where(causal, scores, -1e30), axis=-1).astype(jnp.bfloat16)
    attn_mixed = jnp.einsum("bhqk,bkhd->bqhd", attn_probs, qkv_proj[:, :, 2], preferred_element_type=jnp.float32).astype(jnp.bfloat16)
    attn_out = jnp.einsum("bsn,nm->bsm", attn_mixed.reshape(n_batch, seq_len, n_heads * HEAD_DIM), out_weight, preferred_element_type=jnp.float32)
    return (x_in.astype(jnp.float32) + attn_out).astype(jnp.bfloat16)


def capacity_for(n_tokens, top_k, n_experts):
    return ((5 * n_tokens * top_k) // (4 * n_experts) + 7) // 8 * 8


def nt_dot(lhs, rhs):
    return lax.dot_general(lhs, rhs, (((1,), (1,)), ((), ())), preferred_element_type=jnp.float32)


def exchange_kernel(n_chunk, spread_in, rows_in, gate_h, rest_h, out, r1, r2, r3, b1, b2, own, inp, spread, rows, w13, w2, xin, inner, yall, w_sem, in_sem, tx, rx, fin, ld):
    f, x, core = lax.axis_index("fsdp"), lax.axis_index("x"), lax.axis_index("core")
    z, y = f // 4, f % 4
    copy = pltpu.make_async_copy

    def dev(axis, hop):
        d = [0, 0, 0]
        d[axis % 3] = hop + 4
        return {"fsdp": (z + d[1]) % 4 * 4 + (y + d[2]) % 4, "x": (x + d[0]) % 4, "core": core}

    def send(src, dst, ssem, rsem, to):
        pltpu.make_async_remote_copy(src_ref=src, dst_ref=dst, send_sem=ssem, recv_sem=rsem, device_id=to, device_id_type=pl.DeviceIdType.MESH).start()

    def wait(ref, sem):
        copy(ref, ref, sem).wait()

    def hop1(k):
        for h in (1, 3, 2):
            send(inp.at[k, h], r1.at[k, h - 1], tx.at[0], rx.at[0, k], dev(k, h))

    def hop2(k):
        wait(r1.at[k], rx.at[0, k])
        for h in (1, 3, 2):
            to = dev(k + 1, h)
            send(r1.at[k, :, h], r2.at[k, h - 1, pl.ds(1, 3)], tx.at[1], rx.at[1, k], to)
            send(inp.at[k, 0, h], r2.at[k, h - 1, 0], tx.at[1], rx.at[1, k], to)

    def hop3(k):
        wait(r2.at[k], rx.at[1, k])
        for h in (1, 3, 2):
            to = dev(k + 2, h)
            send(r2.at[k, :, :, h], r3.at[k, h - 1, pl.ds(1, 3)], tx.at[2], rx.at[2, k], to)
            send(r1.at[k, :, 0, h], r3.at[k, h - 1, 0, pl.ds(1, 3)], tx.at[2], rx.at[2, k], to)
            send(inp.at[k, 0, 0, h], r3.at[k, h - 1, 0, 0], tx.at[2], rx.at[2, k], to)

    def back2(k):
        wait(b1.at[k], rx.at[3, k])
        for h in (1, 3, 2):
            to = dev(k + 1, -h)
            send(b1.at[k, :, h, pl.ds(1, 3)], b2.at[k, h - 1, pl.ds(1, 3)], tx.at[4], rx.at[4, k], to)
            send(own.at[k, h, pl.ds(1, 3)], b2.at[k, h - 1, 0], tx.at[4], rx.at[4, k], to)
            send(b1.at[k, :, h, 0], out.at[k, 0, h, pl.ds(1, 3)], tx.at[5], fin.at[1], to)
            send(own.at[k, h, 0], out.at[k, 0, h, 0], tx.at[5], fin.at[1], to)

    def back3(k):
        wait(b2.at[k], rx.at[4, k])
        for h in (1, 3, 2):
            to = dev(k, -h)
            send(b2.at[k, :, :, h - 1], out.at[k, h, pl.ds(1, 3)], tx.at[6], fin.at[0], to)
            send(b1.at[k, :, 0, h], out.at[k, h, 0, pl.ds(1, 3)], tx.at[6], fin.at[0], to)
            send(own.at[k, 0, h], out.at[k, h, 0, 0], tx.at[6], fin.at[0], to)

    def load(k):
        wait(r3.at[k], rx.at[2, k])
        copy(r3.at[k], xin.at[pl.ds(1, 3)], in_sem).start()
        copy(r2.at[k, :, :, 0], xin.at[0, pl.ds(1, 3)], in_sem).start()
        copy(r1.at[k, :, 0, 0], xin.at[0, 0, pl.ds(1, 3)], in_sem).start()
        copy(inp.at[k, 0, 0, 0], xin.at[0, 0, 0], in_sem).start()
        wait(xin, in_sem)

    n_tile = gate_h.shape[2] // 128

    def experts(k):
        load(k)
        rows = xin.shape[0] * xin.shape[1] * xin.shape[2] * xin.shape[3]

        def up_tile(j, carry):
            lhs = xin[...].reshape(rows, xin.shape[4])
            cols = w13[:, :, :, pl.ds(pl.multiple_of(j * 256, 256), 256)].reshape(-1, 256)
            both = jnp.dot(lhs, cols, preferred_element_type=jnp.float32)
            act = jax.nn.silu(both[:, :128]) * both[:, 128:]
            inner[:, pl.ds(pl.multiple_of(j * 128, 128), 128)] = act.astype(jnp.bfloat16)
            return carry

        lax.fori_loop(0, n_tile, up_tile, 0)

        def down_tile(n, carry):
            rhs = w2[pl.ds(n * 2, 2)].reshape(256, w2.shape[3])
            res = lax.dot_general(inner[...], rhs, (((1,), (1,)), ((), ())), preferred_element_type=jnp.float32)
            yall[k, :, :, :, :, pl.ds(pl.multiple_of(n * 256, 256), 256)] = res.astype(jnp.bfloat16).reshape(4, 4, 4, 8, 256)
            return carry

        lax.fori_loop(0, w2.shape[0] // 2, down_tile, 0)

    def back1(k):
        copy(yall.at[k, 0], own.at[k], ld.at[0, k]).start()
        copy(yall.at[k, 0, 0, 0], out.at[k, 0, 0, 0], ld.at[1, k]).start()
        for h in (1, 3, 2):
            to = dev(k + 2, -h)
            send(yall.at[k, h], b1.at[k, h - 1], tx.at[3], rx.at[3, k], to)
            send(yall.at[k, h, 0, 0], out.at[k, 0, 0, h], tx.at[7], fin.at[2], to)

    def landed(k):
        wait(own.at[k], ld.at[0, k])
        wait(out.at[k, 0, 0, 0], ld.at[1, k])

    def place(k):
        block = spread[pl.ds(k * per_chunk, per_chunk), :]
        for n in range(rows.shape[1] // 512):
            cols = pl.ds(n * 512, 512)
            picked = jnp.dot(block, rows[:, cols], preferred_element_type=jnp.float32)
            inp[k, :, :, :, :, cols] = picked.astype(jnp.bfloat16).reshape(inp.shape[1:5] + (512,))

    per_chunk = spread.shape[0] // n_chunk
    partner = {"core": 1 - core}
    copy(rows_in, rows, ld.at[0, 0]).start()
    copy(spread_in, spread, ld.at[1, 0]).start()
    barrier = pltpu.get_barrier_semaphore()
    for axis in range(3):
        for h in (1, 2, 3):
            pl.semaphore_signal(barrier, inc=1, device_id=dev(axis, h), device_id_type=pl.DeviceIdType.MESH)
    pl.semaphore_signal(barrier, inc=1, device_id=partner, device_id_type=pl.DeviceIdType.MESH)
    wait(rows, ld.at[0, 0])
    wait(spread, ld.at[1, 0])
    place(0)
    pl.semaphore_wait(barrier, 10)
    hop1(0)
    place(1)
    hop1(1)
    place(2)
    hop1(2)
    for part, half in enumerate((gate_h, rest_h)):
        for j in range(n_tile):
            src = half.at[:, :, pl.ds(j * 128, 128)]
            dst = w13.at[:, core, :, pl.ds(j * 256 + part * 128, 128)]
            copy(src, dst, w_sem.at[0]).start()
            send(src, dst, w_sem.at[2], w_sem.at[4], partner)
    down_h = rest_h.at[:, :, pl.ds(n_tile * 128, n_tile * 128)]
    copy(down_h, w2.at[:, core], w_sem.at[1]).start()
    send(down_h, w2.at[:, core], w_sem.at[3], w_sem.at[5], partner)
    for k in (4, 5, 3):
        place(k)
        if k != 3:
            hop1(k)
    hop2(0)
    hop2(1)
    hop2(2)
    hop1(3)
    hop3(2)
    hop2(5)
    hop2(4)
    hop3(0)
    hop2(3)
    hop3(1)
    hop3(4)
    for i in (0, 2, 4):
        wait(w13.at[:, 0], w_sem.at[i])
    for i in (1, 3, 5):
        wait(w2.at[:, 0], w_sem.at[i])

    def turn(k):
        experts(k)
        back1(k)

    def fold(k):
        landed(k)
        back2(k)

    turn(2)
    hop3(5)
    hop3(3)
    for k in (0, 1, 3):
        turn(k)
    fold(2)
    fold(0)
    turn(4)
    fold(1)
    turn(5)
    back3(0)
    fold(3)
    back3(2)
    fold(5)
    back3(1)
    fold(4)
    for k in (5, 4, 3):
        back3(k)

    wait(out.at[:, pl.ds(1, 3)], tx.at[6])
    wait(out.at[:, 0, pl.ds(1, 3)], tx.at[5])
    wait(out.at[:, 0, 0, pl.ds(1, 3)], tx.at[7])
    for ref, i in ((r1, 0), (r2, 1), (r3, 2), (b1, 3), (b2, 4)):
        wait(ref, tx.at[i])
    wait(out.at[:, pl.ds(1, 3)], fin.at[0])
    wait(out.at[:, 0, pl.ds(1, 3)], fin.at[1])
    wait(out.at[:, 0, 0, pl.ds(1, 3)], fin.at[2])


def run_exchange(spread, rows, gate_h, rest_h):
    blk, dim = 8, rows.shape[1]
    n_chunk = spread.shape[0] // (64 * blk)
    width = gate_h.shape[2]
    bf = jnp.bfloat16
    shapes = [(4, 4, 4), (3, 4, 4), (3, 4, 4), (3, 4, 4), (3, 4, 4), (3, 4, 3), (4, 4)]
    outs = pl.pallas_call(
        functools.partial(exchange_kernel, n_chunk),
        out_shape=[jax.ShapeDtypeStruct((n_chunk,) + sh + (blk, dim), bf) for sh in shapes],
        in_specs=[pl.BlockSpec(memory_space=pl.ANY)] * 4,
        out_specs=[pl.BlockSpec(memory_space=pl.ANY)] * len(shapes),
        scratch_shapes=[
            pltpu.VMEM((n_chunk, 4, 4, 4, blk, dim), bf),
            pltpu.VMEM(spread.shape, bf),
            pltpu.VMEM(rows.shape, bf),
            pltpu.VMEM((16, 2, 64, 2 * width), bf),
            pltpu.VMEM((16, 2, 64, width), bf),
            pltpu.VMEM((4, 4, 4, blk, dim), bf),
            pltpu.VMEM((64 * blk, width), bf),
            pltpu.VMEM((n_chunk, 4, 4, 4, blk, dim), bf),
            pltpu.SemaphoreType.DMA((6,)),
            pltpu.SemaphoreType.DMA,
            pltpu.SemaphoreType.DMA((8,)),
            pltpu.SemaphoreType.DMA((5, n_chunk)),
            pltpu.SemaphoreType.DMA((3,)),
            pltpu.SemaphoreType.DMA((2, n_chunk)),
        ],
        compiler_params=pltpu.CompilerParams(has_side_effects=True, collective_id=0, vmem_limit_bytes=60 * 2**20),
        name="expert_exchange",
    )(spread, rows, gate_h, rest_h)
    return outs[0]


def solution(mesh):
    n_f, n_ep = mesh.shape["fsdp"], mesh.shape["ep"]
    n_core = 2
    n_x = n_ep // n_core
    phys = Mesh(mesh.devices.reshape(n_f, n_x, n_core), ALL)
    tok_spec = P(ALL)
    row_spec = P("fsdp", None)
    ep = ("x", "core")

    def gather_rows(*shards):
        part = shards[0].shape[0] // n_ep
        mine = lax.axis_index("x") * n_core + lax.axis_index("core")
        piece = jnp.concatenate([lax.dynamic_slice_in_dim(shard, mine * part, part, 0) for shard in shards], axis=1)
        return lax.all_gather(piece, ALL, axis=0, tiled=True)

    def stage_expert(shard):
        core = lax.axis_index("core")
        half = shard.shape[1] // n_core
        keep = lax.dynamic_slice_in_dim(shard, core * half, half, 1)
        give = lax.dynamic_slice_in_dim(shard, (1 - core) * half, half, 1)
        got = lax.ppermute(give, "core", SWAP)
        first = core == 0
        return jnp.concatenate([jnp.where(first, keep, got), jnp.where(first, got, keep)], axis=0)

    def local_step(x_in, w_qkv, w_out, w_gate, w_up, w_down, ws_gate, ws_up, ws_down, expert_ids, slot_ids, gate_vals):
        n_batch, seq_len, model_dim = x_in.shape
        n_tokens = n_batch * seq_len
        top_k = expert_ids.shape[-1]
        n_experts = w_gate.shape[0] * n_ep
        capacity = capacity_for(n_tokens, top_k, n_experts)
        n_rows = n_experts * capacity
        s_ff = ws_gate.shape[1]

        n_qkv = w_qkv.shape[1]
        n_attn = n_qkv + w_out.shape[1]
        dense = gather_rows(w_qkv, w_out, ws_gate, ws_up, lax.optimization_barrier(ws_down.T))
        gate_h = lax.all_to_all(stage_expert(w_gate), "fsdp", 0, 0, tiled=True)
        rest = jnp.concatenate([stage_expert(w_up), stage_expert(jnp.swapaxes(w_down, 1, 2))], axis=2)
        dense, rest, gate_h = lax.optimization_barrier((dense, rest, gate_h))
        rest_h = lax.all_to_all(rest, "fsdp", 0, 0, tiled=True)
        qkv_full, out_full, shared_full = dense[:, :n_qkv], dense[:, n_qkv:n_attn], dense[:, n_attn:]

        ids = expert_ids.reshape(n_tokens, top_k)
        slots = slot_ids.reshape(n_tokens, top_k)
        gates = gate_vals.reshape(n_tokens, top_k)
        kept = slots >= 0
        far, chip = lax.axis_index("fsdp"), lax.axis_index("x")
        rel_x = (ids // n_f - chip) % 4
        rel_z = (ids % n_f // 4 - far // 4) % 4
        rel_y = (ids % 4 - far % 4) % 4
        turn = slots // 8 % 3
        hop_a = jnp.where(turn == 0, rel_x, jnp.where(turn == 1, rel_z, rel_y))
        hop_b = jnp.where(turn == 0, rel_z, jnp.where(turn == 1, rel_y, rel_x))
        hop_c = jnp.where(turn == 0, rel_y, jnp.where(turn == 1, rel_x, rel_z))
        row = ((slots // 8 * 4 + hop_a) * 4 + hop_b) * 4 + hop_c
        row = jnp.where(kept, row * 8 + slots % 8, n_rows).reshape(-1)
        source_tok = jnp.arange(n_tokens * top_k, dtype=jnp.int32) // top_k
        tok_iota = jnp.arange(n_tokens, dtype=jnp.int32)
        row_source = jnp.full((n_rows,), n_tokens, jnp.int32).at[row].set(source_tok, mode="drop")
        row_gate = jnp.zeros((n_rows,), gates.dtype).at[row].set(gates.reshape(-1), mode="drop")
        spread = (row_source[:, None] == tok_iota[None, :]).astype(jnp.bfloat16)
        merge = jnp.where(row_source[None, :] == tok_iota[:, None], row_gate[None, :], jnp.zeros((), gates.dtype))

        hidden = attention_block(x_in, qkv_full, out_full).reshape(n_tokens, model_dim)
        normed = rms_norm(hidden)
        s_gate = jnp.dot(normed, shared_full[:, :s_ff], preferred_element_type=jnp.float32)
        s_up = jnp.dot(normed, shared_full[:, s_ff:2 * s_ff], preferred_element_type=jnp.float32)
        s_inner = (jax.nn.silu(s_gate) * s_up).astype(jnp.bfloat16)
        shared_out = nt_dot(s_inner, shared_full[:, 2 * s_ff:])
        routed_rows, shared_out = lax.optimization_barrier((normed, shared_out))
        back = run_exchange(spread, routed_rows, gate_h, rest_h)
        routed = jnp.dot(merge, back.reshape(n_rows, model_dim), preferred_element_type=jnp.float32)

        summed = hidden.astype(jnp.float32) + shared_out + routed
        return summed.astype(jnp.bfloat16).reshape(n_batch, seq_len, model_dim)

    return jax.shard_map(local_step, mesh=phys, in_specs=(tok_spec, row_spec, row_spec, P(ep, "fsdp", None), P(ep, "fsdp", None), P(ep, None, "fsdp"), row_spec, row_spec, P(None, "fsdp"), tok_spec, tok_spec, tok_spec), out_specs=tok_spec, check_vma=False)
```

```python
import functools

import jax
import jax.numpy as jnp
from jax import lax
from jax.experimental import pallas as pl
from jax.experimental.pallas import tpu as pltpu
from jax.sharding import Mesh, PartitionSpec as P


HEAD_DIM = 128
ROPE_BASE = 10000.0
EPSILON = 1e-6
ALL = ("fsdp", "x", "core")
SWAP = [(0, 1), (1, 0)]


def rms_norm(values):
    vals_f32 = values.astype(jnp.float32)
    mean_sq = jnp.mean(vals_f32 * vals_f32, axis=-1, keepdims=True)
    return (vals_f32 * lax.rsqrt(mean_sq + EPSILON)).astype(jnp.bfloat16)


def attention_kernel(q_ref, k_ref, v_ref, cos_ref, sin_ref, out_ref):
    seq_len, width = q_ref.shape
    cos_tab, sin_tab = cos_ref[...], sin_ref[...]
    block = 128

    def rotate(vals):
        vals_f32 = vals.astype(jnp.float32)
        return (vals_f32 * cos_tab + pltpu.roll(vals_f32, HEAD_DIM // 2, 1) * sin_tab).astype(jnp.bfloat16)

    for h in range(width // HEAD_DIM):
        cols = slice(h * HEAD_DIM, (h + 1) * HEAD_DIM)
        query, key, value = rotate(q_ref[:, cols]), rotate(k_ref[:, cols]), v_ref[:, cols]
        for i in range(seq_len // block):
            seen = (i + 1) * block
            scores = lax.dot_general(query[i * block:seen], key[:seen], (((1,), (1,)), ((), ())), preferred_element_type=jnp.float32) * (HEAD_DIM ** -0.5)
            row = lax.broadcasted_iota(jnp.int32, scores.shape, 0) + i * block
            scores = jnp.where(row >= lax.broadcasted_iota(jnp.int32, scores.shape, 1), scores, -1e30)
            weights = jnp.exp(scores - jnp.max(scores, axis=-1, keepdims=True))
            probs = (weights / jnp.sum(weights, axis=-1, keepdims=True)).astype(jnp.bfloat16)
            mixed = jnp.dot(probs, value[:seen], preferred_element_type=jnp.float32)
            out_ref[i * block:seen, cols] = mixed.astype(jnp.bfloat16)


def attention_block(x_in, qkv_weight, out_weight):
    _, seq_len, model_dim = x_in.shape
    n_heads = qkv_weight.shape[1] // (3 * HEAD_DIM)
    half_dim = HEAD_DIM // 2
    tokens = x_in.reshape(seq_len, model_dim)
    normed = rms_norm(tokens)
    qkv_proj = jnp.dot(normed, qkv_weight, preferred_element_type=jnp.float32).astype(jnp.bfloat16)
    positions = jnp.arange(seq_len, dtype=jnp.float32)
    inv_freq = ROPE_BASE ** (-jnp.arange(half_dim, dtype=jnp.float32) * (2.0 / HEAD_DIM))
    angles = positions[:, None] * inv_freq[None, :]
    cos_tab, sin_tab = jnp.cos(angles), jnp.sin(angles)
    cos_tab = jnp.concatenate([cos_tab, cos_tab], axis=1)
    sin_tab = jnp.concatenate([-sin_tab, sin_tab], axis=1)
    pair = 2 * HEAD_DIM
    steps = n_heads // 2
    attn_mixed = pl.pallas_call(
        attention_kernel,
        out_shape=jax.ShapeDtypeStruct((seq_len, n_heads * HEAD_DIM), jnp.bfloat16),
        grid=(steps,),
        in_specs=[
            pl.BlockSpec((seq_len, pair), lambda h: (0, h)),
            pl.BlockSpec((seq_len, pair), lambda h: (0, h + steps)),
            pl.BlockSpec((seq_len, pair), lambda h: (0, h + 2 * steps)),
            pl.BlockSpec((seq_len, HEAD_DIM), lambda h: (0, 0)),
            pl.BlockSpec((seq_len, HEAD_DIM), lambda h: (0, 0)),
        ],
        out_specs=pl.BlockSpec((seq_len, pair), lambda h: (0, h)),
        compiler_params=pltpu.CompilerParams(vmem_limit_bytes=24 * 2**20),
        cost_estimate=pl.CostEstimate(flops=8 * 10**9, bytes_accessed=7 * 2**20, transcendentals=2 * 10**6),
        name="causal_attention",
    )(qkv_proj, qkv_proj, qkv_proj, cos_tab, sin_tab)
    attn_out = jnp.dot(attn_mixed, out_weight, preferred_element_type=jnp.float32)
    return (tokens.astype(jnp.float32) + attn_out).astype(jnp.bfloat16)


def capacity_for(n_tokens, top_k, n_experts):
    return ((5 * n_tokens * top_k) // (4 * n_experts) + 7) // 8 * 8


def nt_dot(lhs, rhs):
    return lax.dot_general(lhs, rhs, (((1,), (1,)), ((), ())), preferred_element_type=jnp.float32)


def exchange_kernel(n_chunk, spread_in, rows_in, fore_h, rest_h, out, r1, r2, r3, b1, b2, own, inp, spread, rows, w13, w2, xin, inner, yall, w_sem, in_sem, tx, rx, fin, ld):
    f, x, core = lax.axis_index("fsdp"), lax.axis_index("x"), lax.axis_index("core")
    z, y = f // 4, f % 4
    copy = pltpu.make_async_copy

    def dev(axis, hop):
        d = [0, 0, 0]
        d[axis % 3] = hop + 4
        return {"fsdp": (z + d[1]) % 4 * 4 + (y + d[2]) % 4, "x": (x + d[0]) % 4, "core": core}

    def send(src, dst, ssem, rsem, to):
        pltpu.make_async_remote_copy(src_ref=src, dst_ref=dst, send_sem=ssem, recv_sem=rsem, device_id=to, device_id_type=pl.DeviceIdType.MESH).start()

    def wait(ref, sem):
        copy(ref, ref, sem).wait()

    def hop1(k):
        for h in (1, 3, 2):
            send(inp.at[k, h], r1.at[k, h - 1], tx.at[0], rx.at[0, k], dev(k, h))

    def hop2(k):
        wait(r1.at[k], rx.at[0, k])
        for h in (1, 3, 2):
            to = dev(k + 1, h)
            send(r1.at[k, :, h], r2.at[k, h - 1, pl.ds(1, 3)], tx.at[1], rx.at[1, k], to)
            send(inp.at[k, 0, h], r2.at[k, h - 1, 0], tx.at[1], rx.at[1, k], to)

    def hop3(k):
        wait(r2.at[k], rx.at[1, k])
        for h in (1, 3, 2):
            to = dev(k + 2, h)
            send(r2.at[k, :, :, h], r3.at[k, h - 1, pl.ds(1, 3)], tx.at[2], rx.at[2, k], to)
            send(r1.at[k, :, 0, h], r3.at[k, h - 1, 0, pl.ds(1, 3)], tx.at[2], rx.at[2, k], to)
            send(inp.at[k, 0, 0, h], r3.at[k, h - 1, 0, 0], tx.at[2], rx.at[2, k], to)

    def back2(k):
        wait(b1.at[k], rx.at[3, k])
        for h in (1, 3, 2):
            to = dev(k + 1, -h)
            send(b1.at[k, :, h, pl.ds(1, 3)], b2.at[k, h - 1, pl.ds(1, 3)], tx.at[4], rx.at[4, k], to)
            send(own.at[k, h, pl.ds(1, 3)], b2.at[k, h - 1, 0], tx.at[4], rx.at[4, k], to)
            send(b1.at[k, :, h, 0], out.at[k, 0, h, pl.ds(1, 3)], tx.at[5], fin.at[1], to)
            send(own.at[k, h, 0], out.at[k, 0, h, 0], tx.at[5], fin.at[1], to)

    def back3(k):
        wait(b2.at[k], rx.at[4, k])
        for h in (1, 3, 2):
            to = dev(k, -h)
            send(b2.at[k, :, :, h - 1], out.at[k, h, pl.ds(1, 3)], tx.at[6], fin.at[0], to)
            send(b1.at[k, :, 0, h], out.at[k, h, 0, pl.ds(1, 3)], tx.at[6], fin.at[0], to)
            send(own.at[k, 0, h], out.at[k, h, 0, 0], tx.at[6], fin.at[0], to)

    def load(k):
        wait(r3.at[k], rx.at[2, k])
        copy(r3.at[k], xin.at[pl.ds(1, 3)], in_sem).start()
        copy(r2.at[k, :, :, 0], xin.at[0, pl.ds(1, 3)], in_sem).start()
        copy(r1.at[k, :, 0, 0], xin.at[0, 0, pl.ds(1, 3)], in_sem).start()
        copy(inp.at[k, 0, 0, 0], xin.at[0, 0, 0], in_sem).start()
        wait(xin, in_sem)

    n_fore = fore_h.shape[2] // 128
    n_tile = (n_fore + rest_h.shape[2] // 128) // 3

    def experts(k):
        load(k)
        rows = xin.shape[0] * xin.shape[1] * xin.shape[2] * xin.shape[3]

        def up_tile(j, carry):
            lhs = xin[...].reshape(rows, xin.shape[4])
            cols = w13[:, :, :, pl.ds(pl.multiple_of(j * 256, 256), 256)].reshape(-1, 256)
            both = jnp.dot(lhs, cols, preferred_element_type=jnp.float32)
            act = jax.nn.silu(both[:, :128]) * both[:, 128:]
            inner[:, pl.ds(pl.multiple_of(j * 128, 128), 128)] = act.astype(jnp.bfloat16)
            return carry

        lax.fori_loop(0, n_tile, up_tile, 0)

        def down_tile(n, carry):
            rhs = w2[pl.ds(n * 2, 2)].reshape(256, w2.shape[3])
            res = lax.dot_general(inner[...], rhs, (((1,), (1,)), ((), ())), preferred_element_type=jnp.float32)
            yall[k, :, :, :, :, pl.ds(pl.multiple_of(n * 256, 256), 256)] = res.astype(jnp.bfloat16).reshape(4, 4, 4, 8, 256)
            return carry

        lax.fori_loop(0, w2.shape[0] // 2, down_tile, 0)

    def back1(k):
        copy(yall.at[k, 0], own.at[k], ld.at[0, k]).start()
        copy(yall.at[k, 0, 0, 0], out.at[k, 0, 0, 0], ld.at[1, k]).start()
        for h in (1, 3, 2):
            to = dev(k + 2, -h)
            send(yall.at[k, h], b1.at[k, h - 1], tx.at[3], rx.at[3, k], to)
            send(yall.at[k, h, 0, 0], out.at[k, 0, 0, h], tx.at[7], fin.at[2], to)

    def landed(k):
        wait(own.at[k], ld.at[0, k])
        wait(out.at[k, 0, 0, 0], ld.at[1, k])

    def place(k):
        block = spread[pl.ds(k * per_chunk, per_chunk), :]
        for n in range(rows.shape[1] // 512):
            cols = pl.ds(n * 512, 512)
            picked = jnp.dot(block, rows[:, cols], preferred_element_type=jnp.float32)
            inp[k, :, :, :, :, cols] = picked.astype(jnp.bfloat16).reshape(inp.shape[1:5] + (512,))

    per_chunk = spread.shape[0] // n_chunk
    partner = {"core": 1 - core}
    copy(rows_in, rows, ld.at[0, 0]).start()
    copy(spread_in, spread, ld.at[1, 0]).start()
    barrier = pltpu.get_barrier_semaphore()
    for axis in range(3):
        for h in (1, 2, 3):
            pl.semaphore_signal(barrier, inc=1, device_id=dev(axis, h), device_id_type=pl.DeviceIdType.MESH)
    pl.semaphore_signal(barrier, inc=1, device_id=partner, device_id_type=pl.DeviceIdType.MESH)
    wait(rows, ld.at[0, 0])
    wait(spread, ld.at[1, 0])
    place(0)
    pl.semaphore_wait(barrier, 10)
    hop1(0)
    place(1)
    hop1(1)
    place(2)
    hop1(2)
    for t in range(2 * n_tile):
        half, at = (fore_h, t) if t < n_fore else (rest_h, t - n_fore)
        src = half.at[:, :, pl.ds(at * 128, 128)]
        dst = w13.at[:, core, :, pl.ds(t % n_tile * 256 + t // n_tile * 128, 128)]
        copy(src, dst, w_sem.at[0]).start()
        send(src, dst, w_sem.at[2], w_sem.at[4], partner)
    down_h = rest_h.at[:, :, pl.ds((2 * n_tile - n_fore) * 128, n_tile * 128)]
    copy(down_h, w2.at[:, core], w_sem.at[1]).start()
    send(down_h, w2.at[:, core], w_sem.at[3], w_sem.at[5], partner)
    for k in (4, 5, 3):
        place(k)
        if k != 3:
            hop1(k)
    hop2(0)
    hop2(1)
    hop2(2)
    hop1(3)
    hop3(2)
    hop2(5)
    hop2(4)
    hop3(0)
    hop2(3)
    hop3(1)
    hop3(4)
    for i in (0, 2, 4):
        wait(w13.at[:, 0], w_sem.at[i])
    for i in (1, 3, 5):
        wait(w2.at[:, 0], w_sem.at[i])

    def turn(k):
        experts(k)
        back1(k)

    def fold(k):
        landed(k)
        back2(k)

    turn(2)
    hop3(5)
    hop3(3)
    for k in (0, 1, 3):
        turn(k)
    fold(2)
    fold(0)
    turn(4)
    fold(1)
    turn(5)
    back3(0)
    fold(3)
    back3(2)
    fold(5)
    back3(1)
    fold(4)
    for k in (5, 4, 3):
        back3(k)

    wait(out.at[:, pl.ds(1, 3)], tx.at[6])
    wait(out.at[:, 0, pl.ds(1, 3)], tx.at[5])
    wait(out.at[:, 0, 0, pl.ds(1, 3)], tx.at[7])
    for ref, i in ((r1, 0), (r2, 1), (r3, 2), (b1, 3), (b2, 4)):
        wait(ref, tx.at[i])
    wait(out.at[:, pl.ds(1, 3)], fin.at[0])
    wait(out.at[:, 0, pl.ds(1, 3)], fin.at[1])
    wait(out.at[:, 0, 0, pl.ds(1, 3)], fin.at[2])


def run_exchange(spread, rows, fore_h, rest_h):
    blk, dim = 8, rows.shape[1]
    n_chunk = spread.shape[0] // (64 * blk)
    width = (fore_h.shape[2] + rest_h.shape[2]) // 3
    bf = jnp.bfloat16
    shapes = [(4, 4, 4), (3, 4, 4), (3, 4, 4), (3, 4, 4), (3, 4, 4), (3, 4, 3), (4, 4)]
    outs = pl.pallas_call(
        functools.partial(exchange_kernel, n_chunk),
        out_shape=[jax.ShapeDtypeStruct((n_chunk,) + sh + (blk, dim), bf) for sh in shapes],
        in_specs=[pl.BlockSpec(memory_space=pl.ANY)] * 4,
        out_specs=[pl.BlockSpec(memory_space=pl.ANY)] * len(shapes),
        scratch_shapes=[
            pltpu.VMEM((n_chunk, 4, 4, 4, blk, dim), bf),
            pltpu.VMEM(spread.shape, bf),
            pltpu.VMEM(rows.shape, bf),
            pltpu.VMEM((16, 2, 64, 2 * width), bf),
            pltpu.VMEM((16, 2, 64, width), bf),
            pltpu.VMEM((4, 4, 4, blk, dim), bf),
            pltpu.VMEM((64 * blk, width), bf),
            pltpu.VMEM((n_chunk, 4, 4, 4, blk, dim), bf),
            pltpu.SemaphoreType.DMA((6,)),
            pltpu.SemaphoreType.DMA,
            pltpu.SemaphoreType.DMA((8,)),
            pltpu.SemaphoreType.DMA((5, n_chunk)),
            pltpu.SemaphoreType.DMA((3,)),
            pltpu.SemaphoreType.DMA((2, n_chunk)),
        ],
        compiler_params=pltpu.CompilerParams(has_side_effects=True, collective_id=0, vmem_limit_bytes=60 * 2**20),
        name="expert_exchange",
    )(spread, rows, fore_h, rest_h)
    return outs[0]


def solution(mesh):
    n_f, n_ep = mesh.shape["fsdp"], mesh.shape["ep"]
    n_core = 2
    n_x = n_ep // n_core
    phys = Mesh(mesh.devices.reshape(n_f, n_x, n_core), ALL)
    tok_spec = P(ALL)
    row_spec = P("fsdp", None)
    ep = ("x", "core")

    def gather_rows(*shards):
        part = shards[0].shape[0] // n_ep
        mine = lax.axis_index("x") * n_core + lax.axis_index("core")
        piece = jnp.concatenate([lax.dynamic_slice_in_dim(shard, mine * part, part, 0) for shard in shards], axis=1)
        return lax.all_gather(piece, ALL, axis=0, tiled=True)

    def stage_expert(shard):
        core = lax.axis_index("core")
        half = shard.shape[1] // n_core
        keep = lax.dynamic_slice_in_dim(shard, core * half, half, 1)
        give = lax.dynamic_slice_in_dim(shard, (1 - core) * half, half, 1)
        got = lax.ppermute(give, "core", SWAP)
        first = core == 0
        return jnp.concatenate([jnp.where(first, keep, got), jnp.where(first, got, keep)], axis=0)

    def local_step(x_in, w_qkv, w_out, w_gate, w_up, w_down, ws_gate, ws_up, ws_down, expert_ids, slot_ids, gate_vals):
        n_batch, seq_len, model_dim = x_in.shape
        n_tokens = n_batch * seq_len
        top_k = expert_ids.shape[-1]
        n_experts = w_gate.shape[0] * n_ep
        capacity = capacity_for(n_tokens, top_k, n_experts)
        n_rows = n_experts * capacity
        s_ff = ws_gate.shape[1]

        n_qkv = w_qkv.shape[1]
        n_attn = n_qkv + w_out.shape[1]
        dense = gather_rows(w_qkv, w_out, ws_gate, ws_up, lax.optimization_barrier(ws_down.T))
        up_half = stage_expert(w_up)
        cut = w_up.shape[2] // 256 * 128
        fore = jnp.concatenate([stage_expert(w_gate), up_half[:, :, :cut]], axis=2)
        rest = jnp.concatenate([up_half[:, :, cut:], stage_expert(jnp.swapaxes(w_down, 1, 2))], axis=2)
        fore_h = lax.all_to_all(fore, "fsdp", 0, 0, tiled=True)
        dense, rest, fore_h = lax.optimization_barrier((dense, rest, fore_h))
        rest_h = lax.all_to_all(rest, "fsdp", 0, 0, tiled=True)
        qkv_full, out_full, shared_full = dense[:, :n_qkv], dense[:, n_qkv:n_attn], dense[:, n_attn:]

        ids = expert_ids.reshape(n_tokens, top_k)
        slots = slot_ids.reshape(n_tokens, top_k)
        gates = gate_vals.reshape(n_tokens, top_k)
        kept = slots >= 0
        far, chip = lax.axis_index("fsdp"), lax.axis_index("x")
        rel_x = (ids // n_f - chip) % 4
        rel_z = (ids % n_f // 4 - far // 4) % 4
        rel_y = (ids % 4 - far % 4) % 4
        turn = slots // 8 % 3
        hop_a = jnp.where(turn == 0, rel_x, jnp.where(turn == 1, rel_z, rel_y))
        hop_b = jnp.where(turn == 0, rel_z, jnp.where(turn == 1, rel_y, rel_x))
        hop_c = jnp.where(turn == 0, rel_y, jnp.where(turn == 1, rel_x, rel_z))
        row = ((slots // 8 * 4 + hop_a) * 4 + hop_b) * 4 + hop_c
        row = jnp.where(kept, row * 8 + slots % 8, n_rows).reshape(-1)
        source_tok = jnp.arange(n_tokens * top_k, dtype=jnp.int32) // top_k
        tok_iota = jnp.arange(n_tokens, dtype=jnp.int32)
        row_source = jnp.full((n_rows,), n_tokens, jnp.int32).at[row].set(source_tok, mode="drop")
        row_gate = jnp.zeros((n_rows,), gates.dtype).at[row].set(gates.reshape(-1), mode="drop")
        spread = (row_source[:, None] == tok_iota[None, :]).astype(jnp.bfloat16)
        merge = jnp.where(row_source[None, :] == tok_iota[:, None], row_gate[None, :], jnp.zeros((), gates.dtype))

        hidden = attention_block(x_in, qkv_full, out_full).reshape(n_tokens, model_dim)
        normed = rms_norm(hidden)
        s_both = jnp.dot(normed, shared_full[:, :2 * s_ff], preferred_element_type=jnp.float32)
        s_gate, s_up = s_both[:, :s_ff], s_both[:, s_ff:]
        s_inner = (jax.nn.silu(s_gate) * s_up).astype(jnp.bfloat16)
        shared_out = nt_dot(s_inner, shared_full[:, 2 * s_ff:])
        routed_rows, shared_out = lax.optimization_barrier((normed, shared_out))
        back = run_exchange(spread, routed_rows, fore_h, rest_h)
        routed = jnp.dot(merge, back.reshape(n_rows, model_dim), preferred_element_type=jnp.float32)

        summed = hidden.astype(jnp.float32) + shared_out + routed
        return summed.astype(jnp.bfloat16).reshape(n_batch, seq_len, model_dim)

    return jax.shard_map(local_step, mesh=phys, in_specs=(tok_spec, row_spec, row_spec, P(ep, "fsdp", None), P(ep, "fsdp", None), P(ep, None, "fsdp"), row_spec, row_spec, P(None, "fsdp"), tok_spec, tok_spec, tok_spec), out_specs=tok_spec, check_vma=False)
```

```python
import functools

import jax
import jax.numpy as jnp
from jax import lax
from jax.experimental import pallas as pl
from jax.experimental.pallas import tpu as pltpu
from jax.sharding import Mesh, PartitionSpec as P


HEAD_DIM = 128
ROPE_BASE = 10000.0
EPSILON = 1e-6
ALL = ("fsdp", "x", "core")
SWAP = [(0, 1), (1, 0)]


def rms_norm(values):
    vals_f32 = values.astype(jnp.float32)
    mean_sq = jnp.mean(vals_f32 * vals_f32, axis=-1, keepdims=True)
    return (vals_f32 * lax.rsqrt(mean_sq + EPSILON)).astype(jnp.bfloat16)


def rotary_embed(heads_in, positions):
    half_dim = HEAD_DIM // 2
    inv_freq = ROPE_BASE ** (-jnp.arange(half_dim, dtype=jnp.float32) * (2.0 / HEAD_DIM))
    angles = positions[:, None] * inv_freq[None, :]
    cos_tab = jnp.cos(angles)[:, None, :]
    sin_tab = jnp.sin(angles)[:, None, :]
    vals_f32 = heads_in.astype(jnp.float32)
    first_half = vals_f32[..., :half_dim]
    second_half = vals_f32[..., half_dim:]
    rotated = jnp.concatenate([first_half * cos_tab - second_half * sin_tab, second_half * cos_tab + first_half * sin_tab], axis=-1)
    return rotated.astype(jnp.bfloat16)


def attention_block(x_in, qkv_weight, out_weight):
    n_batch, seq_len, _ = x_in.shape
    n_heads = qkv_weight.shape[1] // (3 * HEAD_DIM)
    normed = rms_norm(x_in)
    qkv_proj = jnp.einsum("bsd,dn->bsn", normed, qkv_weight, preferred_element_type=jnp.float32).astype(jnp.bfloat16)
    qkv_proj = qkv_proj.reshape(n_batch, seq_len, 3, n_heads, HEAD_DIM)
    positions = jnp.arange(seq_len, dtype=jnp.float32)
    query_rot = rotary_embed(qkv_proj[:, :, 0], positions)
    key_rot = rotary_embed(qkv_proj[:, :, 1], positions)
    scores = jnp.einsum("bqhd,bkhd->bhqk", query_rot, key_rot, preferred_element_type=jnp.float32) * (HEAD_DIM ** -0.5)
    causal = jnp.arange(seq_len)[:, None] >= jnp.arange(seq_len)[None, :]
    attn_probs = jax.nn.softmax(jnp.where(causal, scores, -1e30), axis=-1).astype(jnp.bfloat16)
    attn_mixed = jnp.einsum("bhqk,bkhd->bqhd", attn_probs, qkv_proj[:, :, 2], preferred_element_type=jnp.float32).astype(jnp.bfloat16)
    attn_out = jnp.einsum("bsn,nm->bsm", attn_mixed.reshape(n_batch, seq_len, n_heads * HEAD_DIM), out_weight, preferred_element_type=jnp.float32)
    return (x_in.astype(jnp.float32) + attn_out).astype(jnp.bfloat16)


def capacity_for(n_tokens, top_k, n_experts):
    return ((5 * n_tokens * top_k) // (4 * n_experts) + 7) // 8 * 8


def nt_dot(lhs, rhs):
    return lax.dot_general(lhs, rhs, (((1,), (1,)), ((), ())), preferred_element_type=jnp.float32)


def exchange_kernel(n_chunk, spread_in, rows_in, gate_h, rest_h, out, r1, r2, r3, b1, b2, own, inp, spread, rows, w13, w2, xin, inner, yall, w_sem, in_sem, tx, rx, fin, ld):
    f, x, core = lax.axis_index("fsdp"), lax.axis_index("x"), lax.axis_index("core")
    z, y = f // 4, f % 4
    copy = pltpu.make_async_copy

    def dev(axis, hop):
        d = [0, 0, 0]
        d[axis % 3] = hop + 4
        return {"fsdp": (z + d[1]) % 4 * 4 + (y + d[2]) % 4, "x": (x + d[0]) % 4, "core": core}

    def send(src, dst, ssem, rsem, to):
        pltpu.make_async_remote_copy(src_ref=src, dst_ref=dst, send_sem=ssem, recv_sem=rsem, device_id=to, device_id_type=pl.DeviceIdType.MESH).start()

    def wait(ref, sem):
        copy(ref, ref, sem).wait()

    def hop1(k):
        for h in (1, 3, 2):
            send(inp.at[k, h], r1.at[k, h - 1], tx.at[0], rx.at[0, k], dev(k, h))

    def hop2(k):
        wait(r1.at[k], rx.at[0, k])
        for h in (1, 3, 2):
            to = dev(k + 1, h)
            send(r1.at[k, :, h], r2.at[k, h - 1, pl.ds(1, 3)], tx.at[1], rx.at[1, k], to)
            send(inp.at[k, 0, h], r2.at[k, h - 1, 0], tx.at[1], rx.at[1, k], to)

    def hop3(k):
        wait(r2.at[k], rx.at[1, k])
        for h in (1, 3, 2):
            to = dev(k + 2, h)
            send(r2.at[k, :, :, h], r3.at[k, h - 1, pl.ds(1, 3)], tx.at[2], rx.at[2, k], to)
            send(r1.at[k, :, 0, h], r3.at[k, h - 1, 0, pl.ds(1, 3)], tx.at[2], rx.at[2, k], to)
            send(inp.at[k, 0, 0, h], r3.at[k, h - 1, 0, 0], tx.at[2], rx.at[2, k], to)

    def back2(k):
        wait(b1.at[k], rx.at[3, k])
        for h in (1, 3, 2):
            to = dev(k + 1, -h)
            send(b1.at[k, :, h, pl.ds(1, 3)], b2.at[k, h - 1, pl.ds(1, 3)], tx.at[4], rx.at[4, k], to)
            send(own.at[k, h, pl.ds(1, 3)], b2.at[k, h - 1, 0], tx.at[4], rx.at[4, k], to)
            send(b1.at[k, :, h, 0], out.at[k, 0, h, pl.ds(1, 3)], tx.at[5], fin.at[1], to)
            send(own.at[k, h, 0], out.at[k, 0, h, 0], tx.at[5], fin.at[1], to)

    def back3(k):
        wait(b2.at[k], rx.at[4, k])
        for h in (1, 3, 2):
            to = dev(k, -h)
            send(b2.at[k, :, :, h - 1], out.at[k, h, pl.ds(1, 3)], tx.at[6], fin.at[0], to)
            send(b1.at[k, :, 0, h], out.at[k, h, 0, pl.ds(1, 3)], tx.at[6], fin.at[0], to)
            send(own.at[k, 0, h], out.at[k, h, 0, 0], tx.at[6], fin.at[0], to)

    def load(k):
        wait(r3.at[k], rx.at[2, k])
        copy(r3.at[k], xin.at[pl.ds(1, 3)], in_sem).start()
        copy(r2.at[k, :, :, 0], xin.at[0, pl.ds(1, 3)], in_sem).start()
        copy(r1.at[k, :, 0, 0], xin.at[0, 0, pl.ds(1, 3)], in_sem).start()
        copy(inp.at[k, 0, 0, 0], xin.at[0, 0, 0], in_sem).start()
        wait(xin, in_sem)

    n_tile = gate_h.shape[2] // 128

    def experts(k):
        load(k)
        rows = xin.shape[0] * xin.shape[1] * xin.shape[2] * xin.shape[3]

        def up_tile(j, carry):
            lhs = xin[...].reshape(rows, xin.shape[4])
            cols = w13[:, :, :, pl.ds(pl.multiple_of(j * 256, 256), 256)].reshape(-1, 256)
            both = jnp.dot(lhs, cols, preferred_element_type=jnp.float32)
            act = jax.nn.silu(both[:, :128]) * both[:, 128:]
            inner[:, pl.ds(pl.multiple_of(j * 128, 128), 128)] = act.astype(jnp.bfloat16)
            return carry

        lax.fori_loop(0, n_tile, up_tile, 0)

        def down_tile(n, carry):
            rhs = w2[pl.ds(n * 2, 2)].reshape(256, w2.shape[3])
            res = lax.dot_general(inner[...], rhs, (((1,), (1,)), ((), ())), preferred_element_type=jnp.float32)
            yall[k, :, :, :, :, pl.ds(pl.multiple_of(n * 256, 256), 256)] = res.astype(jnp.bfloat16).reshape(4, 4, 4, 8, 256)
            return carry

        lax.fori_loop(0, w2.shape[0] // 2, down_tile, 0)

    def back1(k):
        copy(yall.at[k, 0], own.at[k], ld.at[0, k]).start()
        copy(yall.at[k, 0, 0, 0], out.at[k, 0, 0, 0], ld.at[1, k]).start()
        for h in (1, 3, 2):
            to = dev(k + 2, -h)
            send(yall.at[k, h], b1.at[k, h - 1], tx.at[3], rx.at[3, k], to)
            send(yall.at[k, h, 0, 0], out.at[k, 0, 0, h], tx.at[7], fin.at[2], to)

    def landed(k):
        wait(own.at[k], ld.at[0, k])
        wait(out.at[k, 0, 0, 0], ld.at[1, k])

    def place(k):
        block = spread[pl.ds(k * per_chunk, per_chunk), :]
        for n in range(rows.shape[1] // 512):
            cols = pl.ds(n * 512, 512)
            picked = jnp.dot(block, rows[:, cols], preferred_element_type=jnp.float32)
            inp[k, :, :, :, :, cols] = picked.astype(jnp.bfloat16).reshape(inp.shape[1:5] + (512,))

    per_chunk = spread.shape[0] // n_chunk
    partner = {"core": 1 - core}
    copy(rows_in, rows, ld.at[0, 0]).start()
    copy(spread_in, spread, ld.at[1, 0]).start()
    barrier = pltpu.get_barrier_semaphore()
    for axis in range(3):
        for h in (1, 2, 3):
            pl.semaphore_signal(barrier, inc=1, device_id=dev(axis, h), device_id_type=pl.DeviceIdType.MESH)
    pl.semaphore_signal(barrier, inc=1, device_id=partner, device_id_type=pl.DeviceIdType.MESH)
    wait(rows, ld.at[0, 0])
    wait(spread, ld.at[1, 0])
    place(0)
    pl.semaphore_wait(barrier, 10)
    hop1(0)
    place(1)
    hop1(1)
    place(2)
    hop1(2)
    for part, half in enumerate((gate_h, rest_h)):
        for j in range(n_tile):
            src = half.at[:, :, pl.ds(j * 128, 128)]
            dst = w13.at[:, core, :, pl.ds(j * 256 + part * 128, 128)]
            copy(src, dst, w_sem.at[0]).start()
            send(src, dst, w_sem.at[2], w_sem.at[4], partner)
    down_h = rest_h.at[:, :, pl.ds(n_tile * 128, n_tile * 128)]
    copy(down_h, w2.at[:, core], w_sem.at[1]).start()
    send(down_h, w2.at[:, core], w_sem.at[3], w_sem.at[5], partner)
    for k in (4, 5, 3):
        place(k)
        if k != 3:
            hop1(k)
    hop2(0)
    hop2(1)
    hop2(2)
    hop1(3)
    hop3(2)
    hop2(5)
    hop2(4)
    hop3(0)
    hop2(3)
    hop3(1)
    hop3(4)
    for i in (0, 2, 4):
        wait(w13.at[:, 0], w_sem.at[i])
    for i in (1, 3, 5):
        wait(w2.at[:, 0], w_sem.at[i])

    def turn(k):
        experts(k)
        back1(k)

    def fold(k):
        landed(k)
        back2(k)

    turn(2)
    hop3(5)
    hop3(3)
    for k in (0, 1, 3):
        turn(k)
    fold(2)
    fold(0)
    turn(4)
    fold(1)
    turn(5)
    back3(0)
    fold(3)
    back3(2)
    fold(5)
    back3(1)
    fold(4)
    for k in (5, 4, 3):
        back3(k)

    wait(out.at[:, pl.ds(1, 3)], tx.at[6])
    wait(out.at[:, 0, pl.ds(1, 3)], tx.at[5])
    wait(out.at[:, 0, 0, pl.ds(1, 3)], tx.at[7])
    for ref, i in ((r1, 0), (r2, 1), (r3, 2), (b1, 3), (b2, 4)):
        wait(ref, tx.at[i])
    wait(out.at[:, pl.ds(1, 3)], fin.at[0])
    wait(out.at[:, 0, pl.ds(1, 3)], fin.at[1])
    wait(out.at[:, 0, 0, pl.ds(1, 3)], fin.at[2])


def run_exchange(spread, rows, gate_h, rest_h):
    blk, dim = 8, rows.shape[1]
    n_chunk = spread.shape[0] // (64 * blk)
    width = gate_h.shape[2]
    bf = jnp.bfloat16
    shapes = [(4, 4, 4), (3, 4, 4), (3, 4, 4), (3, 4, 4), (3, 4, 4), (3, 4, 3), (4, 4)]
    outs = pl.pallas_call(
        functools.partial(exchange_kernel, n_chunk),
        out_shape=[jax.ShapeDtypeStruct((n_chunk,) + sh + (blk, dim), bf) for sh in shapes],
        in_specs=[pl.BlockSpec(memory_space=pl.ANY)] * 4,
        out_specs=[pl.BlockSpec(memory_space=pl.ANY)] * len(shapes),
        scratch_shapes=[
            pltpu.VMEM((n_chunk, 4, 4, 4, blk, dim), bf),
            pltpu.VMEM(spread.shape, bf),
            pltpu.VMEM(rows.shape, bf),
            pltpu.VMEM((16, 2, 64, 2 * width), bf),
            pltpu.VMEM((16, 2, 64, width), bf),
            pltpu.VMEM((4, 4, 4, blk, dim), bf),
            pltpu.VMEM((64 * blk, width), bf),
            pltpu.VMEM((n_chunk, 4, 4, 4, blk, dim), bf),
            pltpu.SemaphoreType.DMA((6,)),
            pltpu.SemaphoreType.DMA,
            pltpu.SemaphoreType.DMA((8,)),
            pltpu.SemaphoreType.DMA((5, n_chunk)),
            pltpu.SemaphoreType.DMA((3,)),
            pltpu.SemaphoreType.DMA((2, n_chunk)),
        ],
        compiler_params=pltpu.CompilerParams(has_side_effects=True, collective_id=0, vmem_limit_bytes=60 * 2**20),
        name="expert_exchange",
    )(spread, rows, gate_h, rest_h)
    return outs[0]


def solution(mesh):
    n_f, n_ep = mesh.shape["fsdp"], mesh.shape["ep"]
    n_core = 2
    n_x = n_ep // n_core
    phys = Mesh(mesh.devices.reshape(n_f, n_x, n_core), ALL)
    tok_spec = P(ALL)
    row_spec = P("fsdp", None)
    ep = ("x", "core")

    def gather_rows(*shards):
        part = shards[0].shape[0] // n_ep
        mine = lax.axis_index("x") * n_core + lax.axis_index("core")
        piece = jnp.concatenate([lax.dynamic_slice_in_dim(shard, mine * part, part, 0) for shard in shards], axis=1)
        return lax.all_gather(piece, ALL, axis=0, tiled=True)

    def stage_expert(shard):
        core = lax.axis_index("core")
        half = shard.shape[1] // n_core
        keep = lax.dynamic_slice_in_dim(shard, core * half, half, 1)
        give = lax.dynamic_slice_in_dim(shard, (1 - core) * half, half, 1)
        got = lax.ppermute(give, "core", SWAP)
        first = core == 0
        return jnp.concatenate([jnp.where(first, keep, got), jnp.where(first, got, keep)], axis=0)

    def local_step(x_in, w_qkv, w_out, w_gate, w_up, w_down, ws_gate, ws_up, ws_down, expert_ids, slot_ids, gate_vals):
        n_batch, seq_len, model_dim = x_in.shape
        n_tokens = n_batch * seq_len
        top_k = expert_ids.shape[-1]
        n_experts = w_gate.shape[0] * n_ep
        capacity = capacity_for(n_tokens, top_k, n_experts)
        n_rows = n_experts * capacity
        s_ff = ws_gate.shape[1]

        n_qkv = w_qkv.shape[1]
        n_attn = n_qkv + w_out.shape[1]
        dense = gather_rows(w_qkv, w_out, ws_gate, ws_up, ws_down.T)
        staged = (stage_expert(w_gate), w_up, w_down, expert_ids, slot_ids, gate_vals)
        gate_half, w_up, w_down, expert_ids, slot_ids, gate_vals = lax.optimization_barrier(staged)
        gate_h = lax.all_to_all(gate_half, "fsdp", 0, 0, tiled=True)
        rest = jnp.concatenate([stage_expert(w_up), stage_expert(jnp.swapaxes(w_down, 1, 2))], axis=2)
        dense, rest, gate_h = lax.optimization_barrier((dense, rest, gate_h))
        rest_h = lax.all_to_all(rest, "fsdp", 0, 0, tiled=True)
        qkv_full, out_full, shared_full = dense[:, :n_qkv], dense[:, n_qkv:n_attn], dense[:, n_attn:]

        ids = expert_ids.reshape(n_tokens, top_k)
        slots = slot_ids.reshape(n_tokens, top_k)
        gates = gate_vals.reshape(n_tokens, top_k)
        kept = slots >= 0
        far, chip = lax.axis_index("fsdp"), lax.axis_index("x")
        rel_x = (ids // n_f - chip) % 4
        rel_z = (ids % n_f // 4 - far // 4) % 4
        rel_y = (ids % 4 - far % 4) % 4
        turn = slots // 8 % 3
        hop_a = jnp.where(turn == 0, rel_x, jnp.where(turn == 1, rel_z, rel_y))
        hop_b = jnp.where(turn == 0, rel_z, jnp.where(turn == 1, rel_y, rel_x))
        hop_c = jnp.where(turn == 0, rel_y, jnp.where(turn == 1, rel_x, rel_z))
        row = ((slots // 8 * 4 + hop_a) * 4 + hop_b) * 4 + hop_c
        row = jnp.where(kept, row * 8 + slots % 8, n_rows).reshape(-1)
        source_tok = jnp.arange(n_tokens * top_k, dtype=jnp.int32) // top_k
        tok_iota = jnp.arange(n_tokens, dtype=jnp.int32)
        row_source = jnp.full((n_rows,), n_tokens, jnp.int32).at[row].set(source_tok, mode="drop")
        row_gate = jnp.zeros((n_rows,), gates.dtype).at[row].set(gates.reshape(-1), mode="drop")
        spread = (row_source[:, None] == tok_iota[None, :]).astype(jnp.bfloat16)
        merge = jnp.where(row_source[None, :] == tok_iota[:, None], row_gate[None, :], jnp.zeros((), gates.dtype))

        hidden = attention_block(x_in, qkv_full, out_full).reshape(n_tokens, model_dim)
        normed = rms_norm(hidden)
        s_gate = jnp.dot(normed, shared_full[:, :s_ff], preferred_element_type=jnp.float32)
        s_up = jnp.dot(normed, shared_full[:, s_ff:2 * s_ff], preferred_element_type=jnp.float32)
        s_inner = (jax.nn.silu(s_gate) * s_up).astype(jnp.bfloat16)
        shared_out = nt_dot(s_inner, shared_full[:, 2 * s_ff:])
        routed_rows, shared_out = lax.optimization_barrier((normed, shared_out))
        back = run_exchange(spread, routed_rows, gate_h, rest_h)
        routed = jnp.dot(merge, back.reshape(n_rows, model_dim), preferred_element_type=jnp.float32)

        summed = hidden.astype(jnp.float32) + shared_out + routed
        return summed.astype(jnp.bfloat16).reshape(n_batch, seq_len, model_dim)

    return jax.shard_map(local_step, mesh=phys, in_specs=(tok_spec, row_spec, row_spec, P(ep, "fsdp", None), P(ep, "fsdp", None), P(ep, None, "fsdp"), row_spec, row_spec, P(None, "fsdp"), tok_spec, tok_spec, tok_spec), out_specs=tok_spec, check_vma=False)
```
